512 devices in a mesh: lon: 64 (over z_lo, y, core), lat: 8 (over x, z_hi).
Axes of the slice: x: 4, y: 8, z: 8 (z_hi: 2, z_lo: 4; z = z_hi * 4 + z_lo), core: 2. Of those that a mesh axis runs over, the one named last changes fastest.
Arguments:
- prediction: bfloat16 [384, 1536, 222], P('lat', 'lon'), may hold values from -40 to 40
- observed_state: bfloat16 [384, 1536, 222], P('lat', 'lon'), may hold values from -40 to 40
- mean_state: bfloat16 [384, 1536, 222], P('lat', 'lon'), may hold values from -6 to 6
- usable_point_flags: int32 [384, 1536], P('lat', 'lon'), may hold values 0 or 1
- eastward_offsets: int32 [8], replicated, may hold values from 0 to 335, as said below
Outputs:
- correlation: float32 [8, 1536, 222], P('lat', 'lon')
The draws below stay inside these ranges and needn't reach their ends.
Inputs may be any that keep to these rules, and one draw needn't show every extreme that they name: `eastward_offsets`: every lag lies below 336, and some lag equals 335.
All inputs are finite; a program needn't handle non-finite values. No bound on the sum of `usable_point_flags` on one device may be relied on, other than what follows from the above.
Results may differ from the reference program's by a relative error of at most 0.0044.
Values may be sent and summed in bfloat16 or wider, within the bound.
No kernel may reach another device: no remote copies, remote signals or barrier semaphores. Data moves between devices by JAX's collectives and lax.ppermute only.
A program may use at most 64 MiB of HBM per device.

```python
import jax
import jax.numpy as jnp
from jax import lax

C = 222
K = 8
REACH = 14
LON_DEV = 24
NLAT = 384
NLON = 1536


def shared_fields(key):
    split_keys = jax.random.split(jax.random.fold_in(key, 7101), 3)
    common = jax.random.normal(split_keys[0], (NLAT, NLON, C), jnp.float32)
    noise_first = jax.random.normal(split_keys[1], (NLAT, NLON, C), jnp.float32)
    noise_second = jax.random.normal(split_keys[2], (NLAT, NLON, C), jnp.float32)
    fore_values = jnp.clip(common + 0.5 * noise_first, -40.0, 40.0)
    true_values = jnp.clip(common + 0.5 * noise_second, -40.0, 40.0)
    return (fore_values, true_values)


def draw_prediction(key, part):
    return shared_fields(key)[0].astype(jnp.bfloat16)


def draw_observed_state(key, part):
    return shared_fields(key)[1].astype(jnp.bfloat16)


def draw_eastward_offsets(key, part):
    split_keys = jax.random.split(jax.random.fold_in(key, 4409), 2)
    values = jax.random.randint(split_keys[0], (K,), 0, REACH * LON_DEV, jnp.int32)
    position = jax.random.randint(split_keys[1], (), 0, K, jnp.int32)
    return values.at[position].set(REACH * LON_DEV - 1)


def with_ends(result, own_key, least, largest):
    index_at = [jax.random.randint(jax.random.fold_in(own_key, axis), (), 0, length) for axis, length in enumerate(result.shape)]
    longest = result.shape.index(max(result.shape))
    beside = index_at[:longest] + [(index_at[longest] + 1) % result.shape[longest]] + index_at[longest + 1:]
    return result.at[tuple(index_at)].set(least).at[tuple(beside)].set(largest)


def block_scale(key, shape, cuts, smallest, largest):
    def one(dim, blocks):
        steps = jax.random.uniform(jax.random.fold_in(jax.random.fold_in(key, 6), dim), (blocks,), jnp.float32, smallest / len(cuts), largest / len(cuts))
        return jnp.repeat(jnp.exp(steps), shape[dim] // blocks).reshape((-1,) + (1,) * (len(shape) - dim - 1))

    factor_of = one(*cuts[0])
    for cut in cuts[1:]:
        factor_of = factor_of * one(*cut)
    return factor_of


def scatter_about(own_key, dims, spread, bound, shards=(), held_as=jnp.bfloat16):
    entries = spread * jax.random.normal(own_key, dims, jnp.float32)
    if shards:
        entries = entries * block_scale(own_key, dims, shards, -0.22, 0.18)
    return jnp.clip(entries, -bound, bound).astype(held_as)


def setup_inputs(seed: int = 0) -> dict:
    seeds = jax.random.split(jax.random.key(seed), 6)
    prediction = draw_prediction(jax.random.fold_in(seeds[5], 71), 0)
    observed_state = draw_observed_state(jax.random.fold_in(seeds[5], 71), 0)
    mean_state = scatter_about(seeds[2], (NLAT, NLON, C), 1.0, 6.0, ((0, 8), (1, 64)))
    usable_point_flags = with_ends((jax.random.randint(seeds[3], (NLAT, NLON), 0, 5) < 4).astype(jnp.int32), jax.random.fold_in(seeds[3], 1), 0, 1)
    eastward_offsets = draw_eastward_offsets(jax.random.fold_in(seeds[5], 71), 0)
    return dict(prediction=prediction, observed_state=observed_state, mean_state=mean_state, usable_point_flags=usable_point_flags, eastward_offsets=eastward_offsets)


regular_term = 0.001

def reference(prediction, observed_state, mean_state, usable_point_flags, eastward_offsets):
    predicted_mean_state = mean_state.astype(jnp.float32)
    prediction_departure = prediction.astype(jnp.float32) - predicted_mean_state
    observed_departure = (observed_state.astype(jnp.float32) - predicted_mean_state).astype(jnp.bfloat16)
    row_index = jnp.arange(NLAT, dtype=jnp.int32).astype(jnp.float32)
    weights = jnp.cos(jnp.pi * ((row_index + 0.5) / NLAT - 0.5))
    valid_f = usable_point_flags.astype(jnp.float32)
    base_weight = weights[:, None] * valid_f
    columns = jnp.arange(NLON, dtype=jnp.int32)

    def one_lag(offset):
        source = ((columns + offset) % NLON).astype(jnp.int32)
        displaced = jnp.take(observed_departure, source, axis=1).astype(jnp.float32)
        shifted_valid = jnp.take(valid_f, source, axis=1)
        couple_factor = (base_weight * shifted_valid)[:, :, None]
        joint_moment = lax.optimization_barrier(jnp.sum(couple_factor * prediction_departure * displaced, axis=0))
        prediction_spread = lax.optimization_barrier(jnp.sum(couple_factor * prediction_departure * prediction_departure, axis=0))
        var_true = lax.optimization_barrier(jnp.sum(couple_factor * displaced * displaced, axis=0))
        return joint_moment / jnp.sqrt((prediction_spread + regular_term) * (var_true + regular_term))
    return lax.map(one_lag, eastward_offsets)
```

```python
import functools

import jax
import jax.numpy as jnp
import numpy as np
from jax import lax
from jax.experimental import pallas as pl
from jax.experimental.pallas import tpu as pltpu
from jax.sharding import Mesh
from jax.sharding import PartitionSpec as P

REG = 0.001
K = 8
ROWS = 48
COLS = 24
CHANNELS = 222
GROUPS = 16
PER = 14
SLOT = 16
SUB = 8
STEPS = ROWS // SUB
BLOCK = GROUPS * COLS
HALO = 14
WINDOW = BLOCK + HALO * COLS
MISSING = 1024.0
LANES = 128


def pack_kernel(field_ref, mean_ref, flags_ref, out_ref, low, mid, high):
    step = pl.program_id(0)
    lane = lax.broadcasted_iota(jnp.int32, (COLS, LANES), 1)
    flags = flags_ref[pl.ds(pl.multiple_of(step * SUB, SUB), SUB), :]
    valid = flags.astype(jnp.float32).T
    pad = jnp.zeros((COLS, 2 * LANES - CHANNELS), jnp.float32)
    for r in range(SUB):
        keep = jnp.broadcast_to(valid[:, r : r + 1], (COLS, LANES)) > 0.5
        left = field_ref[r, :, :LANES].astype(jnp.float32) - mean_ref[r, :, :LANES].astype(jnp.float32)
        right = field_ref[r, :, LANES:].astype(jnp.float32) - mean_ref[r, :, LANES:].astype(jnp.float32)
        left = jnp.where(keep, left, MISSING)
        right = jnp.where(keep, jnp.concatenate([right, pad], axis=1), MISSING)
        low[r] = left
        high[r] = right
        mid[r] = jnp.where(lane >= 9 * PER, left, right)
    for q in range(GROUPS):
        source = low if q < 9 else mid if q == 9 else high
        acc = jnp.full((COLS, LANES), MISSING, jnp.float32)
        for r in range(SUB):
            moved = pltpu.roll(source[r], (SLOT * r - PER * q) % LANES, 1)
            here = (lane >= SLOT * r) & (lane < SLOT * r + PER)
            acc = jnp.where(here, moved, acc)
        out_ref[q] = acc.astype(jnp.bfloat16)


def pack(field, mean, flags):
    return pl.pallas_call(
        pack_kernel,
        grid=(STEPS,),
        in_specs=[
            pl.BlockSpec((SUB, COLS, CHANNELS), lambda i: (i, 0, 0)),
            pl.BlockSpec((SUB, COLS, CHANNELS), lambda i: (i, 0, 0)),
            pl.BlockSpec((ROWS, COLS), lambda i: (0, 0)),
        ],
        out_specs=pl.BlockSpec((GROUPS, COLS, LANES), lambda i: (0, i, 0)),
        out_shape=jax.ShapeDtypeStruct((GROUPS, STEPS * COLS, LANES), jnp.bfloat16),
        scratch_shapes=[pltpu.VMEM((SUB, COLS, LANES), jnp.float32)] * 3,
        cost_estimate=pl.CostEstimate(flops=4_000_000, bytes_accessed=2_000_000, transcendentals=0),
        name="pack",
    )(field, mean, flags)


def sums_kernel(offsets_ref, weight_ref, fore_ref, true_ref, next_ref, gather_ref, out_ref, cross, square, weigh, shifted, usable, total):
    for g in range(STEPS):
        weight = weight_ref[g : g + 1, :]
        rows = pl.ds(g * COLS, COLS)

        def own(p, carry):
            at = pl.ds(pl.multiple_of(g * BLOCK + p * COLS, 8), COLS)
            value = fore_ref[p, rows, :].astype(jnp.float32)
            keep = value < MISSING / 2
            value = jnp.where(keep, value, 0.0)
            masked = jnp.where(keep, weight, 0.0)
            weigh[at, :] = masked
            scaled = value * masked
            cross[at, :] = scaled
            square[at, :] = scaled * value
            return carry

        lax.fori_loop(0, GROUPS, own, 0)

        def other(source, first):
            def run(p, carry):
                at = pl.ds(pl.multiple_of(g * WINDOW + first + p * COLS, 8), COLS)
                value = source[p, rows, :].astype(jnp.float32)
                keep = value < MISSING / 2
                shifted[at, :] = jnp.where(keep, value, 0.0)
                usable[at, :] = jnp.where(keep, 1.0, 0.0)
                return carry

            return run

        lax.fori_loop(0, GROUPS, other(true_ref, 0), 0)
        lax.fori_loop(0, HALO, other(next_ref, BLOCK), 0)

    lag = [offsets_ref[k] for k in range(K)]

    def tile(t, carry):
        for part in range(COLS // 8):
            start = t * COLS + part * 8
            acc = [[jnp.zeros((8, LANES), jnp.float32)] * 3 for _ in range(K)]
            for g in range(STEPS):
                at = pl.ds(pl.multiple_of(g * BLOCK + start, 8), 8)
                a, c, d = cross[at, :], square[at, :], weigh[at, :]
                for k in range(K):
                    there = pl.ds(g * WINDOW + start + lag[k], 8)
                    b, v = shifted[there, :], usable[there, :]
                    acc[k] = [acc[k][0] + a * b, acc[k][1] + c * v, acc[k][2] + d * (b * b)]
            for k in range(K):
                for n in range(3):
                    column = (n * 3 + part) * LANES
                    total[pl.ds(pl.multiple_of((k * GROUPS + t) * 8, 8), 8), column : column + LANES] = acc[k][n]
        return carry

    lax.fori_loop(0, GROUPS, tile, 0)
    whole = total[...]
    first = whole.astype(jnp.bfloat16)
    second = (whole - first.astype(jnp.float32)).astype(jnp.bfloat16)
    gather = gather_ref[...]
    out = jnp.dot(first, gather, preferred_element_type=jnp.float32)
    out += jnp.dot(second, gather, preferred_element_type=jnp.float32)
    out_ref[...] = out.astype(jnp.bfloat16)


def gather_matrix():
    m = np.zeros((9, SUB, SLOT, LANES), np.float32)
    for n in range(9):
        for c in range(PER):
            m[n, :, c, n * PER + c] = 1.0
    return m.reshape(9 * LANES, LANES)


def lag_sums(offsets, weight, fore, true, following):
    vmem = pl.BlockSpec(memory_space=pltpu.VMEM)
    f32 = jnp.float32
    return pl.pallas_call(
        sums_kernel,
        in_specs=[pl.BlockSpec(memory_space=pltpu.SMEM)] + [vmem] * 5,
        out_specs=vmem,
        out_shape=jax.ShapeDtypeStruct((K * GROUPS * 8, LANES), jnp.bfloat16),
        scratch_shapes=[pltpu.VMEM((STEPS * BLOCK, LANES), f32)] * 3
        + [pltpu.VMEM((STEPS * WINDOW, LANES), f32)] * 2
        + [pltpu.VMEM((K * GROUPS * 8, 9 * LANES), f32)],
        cost_estimate=pl.CostEstimate(flops=20_000_000, bytes_accessed=4_000_000, transcendentals=0),
        name="lag_sums",
    )(offsets, weight, fore, true, following, jnp.asarray(gather_matrix(), jnp.bfloat16))


def finish_kernel(parts_ref, out_ref):
    lane = lax.broadcasted_iota(jnp.int32, (8, LANES), 1)
    halves = [[jnp.zeros((8, LANES), jnp.float32)] * 2 for _ in range(3)]
    for q in range(GROUPS):
        total = parts_ref[q].astype(jnp.float32)
        for device in range(1, K):
            total = total + parts_ref[device * GROUPS + q].astype(jnp.float32)
        fore = pltpu.roll(total, LANES - 3 * PER, 1)
        true = pltpu.roll(total, LANES - 6 * PER, 1)
        value = total / jnp.sqrt((fore + REG) * (true + REG))
        low, high = PER * q, PER * q + PER
        for part in range(3):
            moved = pltpu.roll(value, (PER * q - PER * part) % LANES, 1)
            for half in range(2):
                at = lane + half * LANES
                if low < (half + 1) * LANES and high > half * LANES:
                    halves[part][half] = jnp.where((at >= low) & (at < high), moved, halves[part][half])
    for part in range(3):
        out_ref[0, part * 8 : part * 8 + 8, :LANES] = halves[part][0]
        out_ref[0, part * 8 : part * 8 + 8, LANES:] = halves[part][1][:, : CHANNELS - LANES]


def finish(parts):
    vmem = pl.BlockSpec(memory_space=pltpu.VMEM)
    return pl.pallas_call(
        finish_kernel,
        in_specs=[vmem],
        out_specs=vmem,
        out_shape=jax.ShapeDtypeStruct((1, COLS, CHANNELS), jnp.float32),
        name="finish",
    )(parts)


def local(prediction, observed_state, mean_state, usable_point_flags, eastward_offsets):
    row = lax.axis_index("lat") * ROWS + jnp.arange(ROWS, dtype=jnp.int32)
    weight = jnp.cos(jnp.pi * ((row.astype(jnp.float32) + 0.5) / (ROWS * lax.axis_size("lat")) - 0.5))
    weight = jnp.repeat(weight.reshape(STEPS, SUB), SLOT, axis=1)
    around = ("y", "core")
    true = pack(observed_state, mean_state, usable_point_flags)
    true = lax.all_to_all(true, around, 0, 0, tiled=True)
    count = lax.axis_size("z")
    following = lax.ppermute(true[:HALO], "z", [((i + 1) % count, i) for i in range(count)])
    fore = pack(prediction, mean_state, usable_point_flags)
    fore = lax.all_to_all(fore, around, 0, 0, tiled=True)
    sums = lag_sums(eastward_offsets, weight, fore, true, following)
    parts = sums.reshape(K * GROUPS, 8, LANES)
    parts = lax.all_to_all(parts, ("lat",) + around, 0, 0, tiled=True)
    return finish(parts)


def solution(mesh):
    split = Mesh(mesh.devices.reshape(4, 8, 2, 8), ("z", "y", "core", "lat"))
    lon = ("z", "y", "core")
    placed = (P("lat", lon, None), P("lat", lon, None), P("lat", lon, None), P("lat", lon), P())
    return jax.shard_map(local, mesh=split, in_specs=placed, out_specs=P("lat", lon, None), check_vma=False)
```

```python
import jax
import jax.numpy as jnp
from jax import lax
from jax.experimental import pallas as pl
from jax.experimental.pallas import tpu as pltpu
from jax.sharding import Mesh
from jax.sharding import PartitionSpec as P

REG = 0.001
K = 8
ROWS = 48
COLS = 24
CHANNELS = 222
GROUPS = 16
PER = 14
SLOT = 16
SUB = 8
STEPS = ROWS // SUB
BLOCK = GROUPS * COLS
HALO = 14
WINDOW = BLOCK + HALO * COLS
MISSING = 1024.0
LANES = 128


def pack_kernel(field_ref, mean_ref, flags_ref, out_ref, field, mean, low, mid, high, arrived):
    def copies(g):
        rows = pl.ds(g * SUB, SUB)
        return (
            pltpu.make_async_copy(field_ref.at[rows], field.at[rows], arrived.at[0, g]),
            pltpu.make_async_copy(mean_ref.at[rows], mean.at[rows], arrived.at[1, g]),
        )

    for g in range(STEPS):
        for copy in copies(g):
            copy.start()
    lane = lax.broadcasted_iota(jnp.int32, (COLS, LANES), 1)
    valid = flags_ref[...].astype(jnp.float32)
    valid = jnp.concatenate([valid, jnp.zeros((COLS, LANES - ROWS), jnp.float32)], axis=1)
    pad = jnp.zeros((COLS, 2 * LANES - CHANNELS), jnp.float32)

    def group(g, carry):
        for copy in copies(g):
            copy.wait()
        usable = pltpu.roll(valid, LANES - g * SUB, 1)
        for r in range(SUB):
            keep = jnp.broadcast_to(usable[:, r : r + 1], (COLS, LANES)) > 0.5
            row = g * SUB + r
            left = field[row, :, :LANES].astype(jnp.float32) - mean[row, :, :LANES].astype(jnp.float32)
            right = field[row, :, LANES:].astype(jnp.float32) - mean[row, :, LANES:].astype(jnp.float32)
            left = pltpu.roll(jnp.where(keep, left, MISSING), SLOT * r, 1)
            right = pltpu.roll(jnp.where(keep, jnp.concatenate([right, pad], axis=1), MISSING), SLOT * r, 1)
            low[r] = left
            high[r] = right
            mid[r] = jnp.where(((lane - SLOT * r) & (LANES - 1)) >= 9 * PER, left, right)
        for q in range(GROUPS):
            source = low if q < 9 else mid if q == 9 else high
            owner = ((lane - PER * q) & (LANES - 1)) // SLOT
            acc = source[0]
            for r in range(1, SUB):
                acc = jnp.where(owner == r, source[r], acc)
            moved = pltpu.roll(acc, -PER * q % LANES, 1)
            out_ref[q, pl.ds(pl.multiple_of(g * COLS, 8), COLS), :] = moved.astype(jnp.bfloat16)
        return carry

    lax.fori_loop(0, STEPS, group, 0)


def on_chip(mib, flops):
    return dict(
        compiler_params=pltpu.CompilerParams(vmem_limit_bytes=mib * 1024 * 1024),
        cost_estimate=pl.CostEstimate(flops=flops, bytes_accessed=2_000_000, transcendentals=0),
    )


def pack(field, mean, flags):
    vmem, hbm = pl.BlockSpec(memory_space=pltpu.VMEM), pl.BlockSpec(memory_space=pltpu.HBM)
    return pl.pallas_call(
        pack_kernel,
        in_specs=[hbm, hbm, vmem],
        out_specs=vmem,
        out_shape=jax.ShapeDtypeStruct((GROUPS, STEPS * COLS, LANES), jnp.bfloat16),
        scratch_shapes=[pltpu.VMEM((ROWS, COLS, CHANNELS), jnp.bfloat16)] * 2
        + [pltpu.VMEM((SUB, COLS, LANES), jnp.float32)] * 3
        + [pltpu.SemaphoreType.DMA((2, STEPS))],
        name="pack",
        **on_chip(62, 4_000_000),
    )(field, mean, flags)


def totals_at(k, t):
    return pl.ds(pl.multiple_of((k * GROUPS + t) * 8, 8), 8)


def halves_of(value):
    first = value.astype(jnp.bfloat16)
    return first, (value - first.astype(jnp.float32)).astype(jnp.bfloat16)


def gather_matrix(n):
    row = lax.broadcasted_iota(jnp.int32, (3 * LANES, LANES), 0)
    lane = lax.broadcasted_iota(jnp.int32, (3 * LANES, LANES), 1)
    channel = row & (SLOT - 1)
    target = channel + PER * (3 * n + row // LANES)
    return jnp.where((channel < PER) & (lane == target), 1.0, 0.0).astype(jnp.bfloat16)


def dot(a, b):
    return jnp.dot(a, b, preferred_element_type=jnp.float32)


def true_kernel(offsets_ref, weight_ref, true_ref, next_ref, out_ref, usable, square, total):
    def unpack(source, first):
        def run(p, carry):
            for g in range(STEPS):
                at = pl.ds(pl.multiple_of(g * WINDOW + first + p * COLS, 8), COLS)
                value = source[p, g * COLS : (g + 1) * COLS, :].astype(jnp.float32)
                keep = value < MISSING / 2
                square[at, :] = jnp.where(keep, value * value, 0.0)
                if first == 0:
                    usable[at, :] = jnp.where(keep, weight_ref[g : g + 1, :], 0.0)
            return carry

        return run

    lax.fori_loop(0, GROUPS, unpack(true_ref, 0), 0)
    lax.fori_loop(0, HALO, unpack(next_ref, BLOCK), 0)
    lag = [offsets_ref[k] for k in range(K)]

    def tile(t, carry):
        for part in range(COLS // 8):
            start = t * COLS + part * 8
            acc = [jnp.zeros((8, LANES), jnp.float32)] * K
            for g in range(STEPS):
                d = usable[pl.ds(pl.multiple_of(g * WINDOW + start, 8), 8), :]
                for k in range(K):
                    acc[k] = acc[k] + d * square[pl.ds(g * WINDOW + start + lag[k], 8), :]
            for k in range(K):
                total[totals_at(k, t), part * LANES : part * LANES + LANES] = acc[k]
        return carry

    lax.fori_loop(0, GROUPS, tile, 0)
    first, second = halves_of(total[...])
    gather = gather_matrix(2)
    out_ref[...] = (dot(first, gather) + dot(second, gather)).astype(jnp.bfloat16)


def fore_kernel(offsets_ref, weight_ref, fore_ref, true_ref, next_ref, true_sums_ref, out_ref, cross, spread, shifted, usable, total):
    def unpack(source, first):
        def run(p, carry):
            for g in range(STEPS):
                rows = slice(g * COLS, (g + 1) * COLS)
                at = pl.ds(pl.multiple_of(g * WINDOW + first + p * COLS, 8), COLS)
                value = source[p, rows, :].astype(jnp.float32)
                keep = value < MISSING / 2
                shifted[at, :] = jnp.where(keep, value, 0.0)
                usable[at, :] = jnp.where(keep, 1.0, 0.0)
                if first == 0:
                    at = pl.ds(pl.multiple_of(g * BLOCK + p * COLS, 8), COLS)
                    value = jnp.where(keep, fore_ref[p, rows, :].astype(jnp.float32), 0.0)
                    scaled = value * weight_ref[g : g + 1, :]
                    cross[at, :] = scaled
                    spread[at, :] = scaled * value
            return carry

        return run

    lax.fori_loop(0, GROUPS, unpack(true_ref, 0), 0)
    lax.fori_loop(0, HALO, unpack(next_ref, BLOCK), 0)
    lag = [offsets_ref[k] for k in range(K)]

    def tile(t, carry):
        for part in range(COLS // 8):
            start = t * COLS + part * 8
            acc = [[jnp.zeros((8, LANES), jnp.float32)] * 2 for _ in range(K)]
            for g in range(STEPS):
                at = pl.ds(pl.multiple_of(g * BLOCK + start, 8), 8)
                a, c = cross[at, :], spread[at, :]
                for k in range(K):
                    there = pl.ds(g * WINDOW + start + lag[k], 8)
                    acc[k] = [acc[k][0] + a * shifted[there, :], acc[k][1] + c * usable[there, :]]
            for k in range(K):
                for n in range(2):
                    column = (n * 3 + part) * LANES
                    total[totals_at(k, t), column : column + LANES] = acc[k][n]
        return carry

    lax.fori_loop(0, GROUPS, tile, 0)
    first, second = halves_of(total[:, : 3 * LANES])
    gather = gather_matrix(0)
    out = dot(first, gather) + dot(second, gather)
    out += dot(total[:, 3 * LANES :].astype(jnp.bfloat16), gather_matrix(1))
    out_ref[...] = (true_sums_ref[...].astype(jnp.float32) + out).astype(jnp.bfloat16)


def window_call(kernel, inputs, scratch, name, flops):
    vmem = pl.BlockSpec(memory_space=pltpu.VMEM)
    return pl.pallas_call(
        kernel,
        in_specs=[pl.BlockSpec(memory_space=pltpu.SMEM)] + [vmem] * (len(inputs) - 1),
        out_specs=vmem,
        out_shape=jax.ShapeDtypeStruct((K * GROUPS * 8, LANES), jnp.bfloat16),
        scratch_shapes=[pltpu.VMEM((rows, lanes), jnp.float32) for rows, lanes in scratch],
        name=name,
        **on_chip(28, flops),
    )(*inputs)


def finish_kernel(parts_ref, out_ref):
    lane = lax.broadcasted_iota(jnp.int32, (8, LANES), 1)
    halves = [[jnp.zeros((8, LANES), jnp.float32)] * 2 for _ in range(3)]
    for q in range(GROUPS):
        total = parts_ref[q].astype(jnp.float32)
        for device in range(1, K):
            total = total + parts_ref[device * GROUPS + q].astype(jnp.float32)
        fore = pltpu.roll(total, LANES - 3 * PER, 1)
        true = pltpu.roll(total, LANES - 6 * PER, 1)
        value = total / jnp.sqrt((fore + REG) * (true + REG))
        low, high = PER * q, PER * q + PER
        for part in range(3):
            moved = pltpu.roll(value, (PER * q - PER * part) % LANES, 1)
            for half in range(2):
                at = lane + half * LANES
                if low < (half + 1) * LANES and high > half * LANES:
                    halves[part][half] = jnp.where((at >= low) & (at < high), moved, halves[part][half])
    for part in range(3):
        out_ref[0, part * 8 : part * 8 + 8, :LANES] = halves[part][0]
        out_ref[0, part * 8 : part * 8 + 8, LANES:] = halves[part][1][:, : CHANNELS - LANES]


def finish(parts):
    vmem = pl.BlockSpec(memory_space=pltpu.VMEM)
    return pl.pallas_call(
        finish_kernel,
        in_specs=[vmem],
        out_specs=vmem,
        out_shape=jax.ShapeDtypeStruct((1, COLS, CHANNELS), jnp.float32),
        name="finish",
        **on_chip(4, 1_000_000),
    )(parts)


def local(prediction, observed_state, mean_state, usable_point_flags, eastward_offsets):
    row = lax.axis_index("lat") * ROWS + jnp.arange(ROWS, dtype=jnp.int32)
    weight = jnp.cos(jnp.pi * ((row.astype(jnp.float32) + 0.5) / (ROWS * lax.axis_size("lat")) - 0.5))
    weight = jnp.repeat(weight.reshape(STEPS, SUB), SLOT, axis=1)
    flags = usable_point_flags.T
    around = ("y", "core")
    true = pack(observed_state, mean_state, flags)
    true = lax.all_to_all(true, around, 0, 0, tiled=True)
    count = lax.axis_size("z")
    following = lax.ppermute(true[:HALO], "z", [((i + 1) % count, i) for i in range(count)])
    fore = pack(prediction, mean_state, flags)
    fore = lax.all_to_all(fore, around, 0, 0, tiled=True)
    own, window, totals = (STEPS * BLOCK, LANES), (STEPS * WINDOW, LANES), K * GROUPS * 8
    true_sums = window_call(
        true_kernel,
        (eastward_offsets, weight, true, following),
        (window, window, (totals, 3 * LANES)),
        "true_side",
        8_000_000,
    )
    sums = window_call(
        fore_kernel,
        (eastward_offsets, weight, fore, true, following, true_sums),
        (own, own, window, window, (totals, 6 * LANES)),
        "fore_side",
        12_000_000,
    )
    parts = sums.reshape(K * GROUPS, 8, LANES)
    parts = lax.all_to_all(parts, ("lat",) + around, 0, 0, tiled=True)
    return finish(parts)


def solution(mesh):
    split = Mesh(mesh.devices.reshape(4, 8, 2, 8), ("z", "y", "core", "lat"))
    lon = ("z", "y", "core")
    placed = (P("lat", lon, None), P("lat", lon, None), P("lat", lon, None), P("lat", lon), P())
    return jax.shard_map(local, mesh=split, in_specs=placed, out_specs=P("lat", lon, None), check_vma=False)
```

```python
import jax
import jax.numpy as jnp
import numpy as np
from jax import lax
from jax.experimental import pallas as pl
from jax.experimental.pallas import tpu as pltpu
from jax.sharding import Mesh
from jax.sharding import PartitionSpec as P

REG = 0.001
K = 8
ROWS = 48
COLS = 24
TILES = COLS // 8
CHANNELS = 222
GROUPS = 16
PER = 14
SIDE = 9
STEPS = 5
TAIL = ROWS - STEPS * SIDE
PACKED = STEPS * COLS + 8
BLOCK = GROUPS * COLS
HALO = 14
WINDOW = BLOCK + HALO * COLS
MISSING = 1024.0
LANES = 128


def pack_kernel(field_ref, mean_ref, flags_ref, out_ref, field, mean, flags, low, mid, high, packed, arrived, leaving):
    def rows_of(g):
        return pl.ds(g * SIDE, SIDE if g < STEPS else TAIL)

    def fetch(g):
        rows = rows_of(g)
        return (
            pltpu.make_async_copy(field_ref.at[rows], field.at[rows], arrived.at[0, g]),
            pltpu.make_async_copy(mean_ref.at[rows], mean.at[rows], arrived.at[1, g]),
        )

    def leave(g):
        rows = pl.ds(g * COLS, COLS if g < STEPS else 8)
        return pltpu.make_async_copy(packed.at[:, rows, :], out_ref.at[:, rows, :], leaving.at[g])

    fetch_flags = pltpu.make_async_copy(flags_ref, flags, arrived.at[2, 0])
    fetch_flags.start()
    for g in range(STEPS + 1):
        for copy in fetch(g):
            copy.start()
    lane = lax.broadcasted_iota(jnp.int32, (8, LANES), 1)
    pad = jnp.zeros((COLS, 2 * LANES - CHANNELS), jnp.float32)
    fetch_flags.wait()
    valid = flags[...].astype(jnp.float32)

    def anomaly(row, keep):
        left = field[row, :, :LANES].astype(jnp.float32) - mean[row, :, :LANES].astype(jnp.float32)
        right = field[row, :, LANES:].astype(jnp.float32) - mean[row, :, LANES:].astype(jnp.float32)
        keep = jnp.broadcast_to(keep, (COLS, LANES)) > 0.5
        return jnp.where(keep, left, MISSING), jnp.where(keep, jnp.concatenate([right, pad], axis=1), MISSING)

    def place(turn, at, part, left, right):
        left, right = pltpu.roll(left, PER * at, 1), pltpu.roll(right, PER * at, 1)
        low[turn, at, part], high[turn, at, part] = left, right
        mid[turn, at, part] = jnp.where(((lane - PER * at) & (LANES - 1)) >= 9 * PER, left, right)

    def take(g):
        for copy in fetch(g):
            copy.wait()
        count = SIDE if g < STEPS else TAIL
        for row in range(count):
            at = g * SIDE + row
            left, right = anomaly(at, valid[:, at : at + 1])
            for part in range(TILES):
                slot, tile = (row, part) if g < STEPS else (part * TAIL + row, 0)
                rows = slice(part * 8, part * 8 + 8)
                place(g % 2, slot, tile, left[rows], right[rows])

    def emit(g):
        for q in range(GROUPS):
            source = low if q < 9 else mid if q == 9 else high
            slot = (lane - PER * q) & (LANES - 1)
            for part in range(TILES if g < STEPS else 1):
                acc = source[g % 2, 0, part]
                for at in range(1, SIDE):
                    acc = jnp.where(slot >= PER * at, source[g % 2, at, part], acc)
                moved = pltpu.roll(acc, -PER * q % LANES, 1)
                packed[q, pl.ds(g * COLS + part * 8, 8), :] = moved.astype(jnp.bfloat16)
        leave(g).start()

    take(0)
    for g in range(STEPS + 1):
        if g < STEPS:
            take(g + 1)
        emit(g)
    for g in range(STEPS + 1):
        leave(g).wait()


def on_chip(mib, flops):
    return dict(
        compiler_params=pltpu.CompilerParams(vmem_limit_bytes=mib * 1024 * 1024),
        cost_estimate=pl.CostEstimate(flops=flops, bytes_accessed=2_000_000, transcendentals=0),
    )


def pack(field, mean, flags):
    anywhere = pl.BlockSpec(memory_space=pl.ANY)
    return pl.pallas_call(
        pack_kernel,
        in_specs=[anywhere] * 3,
        out_specs=anywhere,
        out_shape=jax.ShapeDtypeStruct((GROUPS, PACKED, LANES), jnp.bfloat16),
        scratch_shapes=[pltpu.VMEM((ROWS, COLS, CHANNELS), jnp.bfloat16)] * 2
        + [pltpu.VMEM((COLS, ROWS), jnp.int32)]
        + [pltpu.VMEM((2, SIDE, TILES, 8, LANES), jnp.float32)] * 3
        + [pltpu.VMEM((GROUPS, PACKED, LANES), jnp.bfloat16)]
        + [pltpu.SemaphoreType.DMA((3, STEPS + 1)), pltpu.SemaphoreType.DMA((STEPS + 1,))],
        name="pack",
        **on_chip(62, 4_000_000),
    )(field, mean, flags)


def totals_at(k, t):
    return pl.ds(pl.multiple_of((t * K + k) * 8, 8), 8)


def halves_of(value):
    first = value.astype(jnp.bfloat16)
    return first, (value - first.astype(jnp.float32)).astype(jnp.bfloat16)


OWN = (STEPS + 1) * BLOCK
OWN_STRIDE = OWN + 8
WINDOW_STRIDE = (STEPS + 1) * WINDOW + 16


def gather_matrix(n):
    row = lax.broadcasted_iota(jnp.int32, (3 * LANES, LANES), 0)
    lane = lax.broadcasted_iota(jnp.int32, (3 * LANES, LANES), 1)
    source = row & (LANES - 1)
    channel = source
    for at in range(1, SIDE + 1):
        channel = jnp.where(source >= PER * at, source - PER * at, channel)
    target = channel + PER * (TILES * n + row // LANES)
    return jnp.where((source < PER * SIDE) & (lane == target), 1.0, 0.0).astype(jnp.bfloat16)


def dot(a, b):
    return jnp.dot(a, b, preferred_element_type=jnp.float32)


def sums_kernel(offsets_ref, weight_ref, fore_ref, true_ref, next_ref, out_ref, held, window, total):
    cross, spread, weigh = (held.at[pl.ds(n * OWN_STRIDE, OWN)] for n in range(3))
    shifted, usable = (window.at[pl.ds(n * WINDOW_STRIDE, (STEPS + 1) * WINDOW)] for n in range(2))
    lane = lax.broadcasted_iota(jnp.int32, (8, LANES), 1)

    def unpack(source, first):
        def tile(g, part, p, value, fore):
            at = pl.ds(pl.multiple_of(g * WINDOW + first + p * COLS + part * 8, 8), 8)
            keep = value < MISSING / 2
            shifted[at, :] = jnp.where(keep, value, 0.0)
            usable[at, :] = jnp.where(keep, 1.0, 0.0)
            if first == 0:
                at = pl.ds(pl.multiple_of(g * BLOCK + p * COLS + part * 8, 8), 8)
                masked = jnp.where(keep, weight_ref[g : g + 1, :], 0.0)
                scaled = fore * masked
                weigh[at, :] = masked
                cross[at, :] = scaled
                spread[at, :] = scaled * fore

        def run(p, carry):
            for g in range(STEPS):
                rows = slice(g * COLS, (g + 1) * COLS)
                value = source[p, rows, :].astype(jnp.float32)
                fore = fore_ref[p, rows, :].astype(jnp.float32) if first == 0 else value
                for part in range(TILES):
                    tile(g, part, p, value[part * 8 : part * 8 + 8], fore[part * 8 : part * 8 + 8])
            rows = slice(STEPS * COLS, PACKED)
            value = source[p, rows, :].astype(jnp.float32)
            fore = fore_ref[p, rows, :].astype(jnp.float32) if first == 0 else value
            for part in range(TILES):
                turn = -PER * TAIL * part % LANES
                moved = pltpu.roll(value, turn, 1) if part else value
                moved = jnp.where(lane < PER * TAIL, moved, MISSING)
                tile(STEPS, part, p, moved, pltpu.roll(fore, turn, 1) if part else fore)
            return carry

        return run

    lax.fori_loop(0, GROUPS, unpack(true_ref, 0), 0, unroll=8)
    lax.fori_loop(0, HALO, unpack(next_ref, BLOCK), 0, unroll=14)
    lag = [offsets_ref[k] for k in range(K)]

    def tile(t, carry):
        for part in range(TILES):
            start = t * COLS + part * 8
            acc = [[jnp.zeros((8, LANES), jnp.float32)] * 3 for _ in range(K)]
            for g in range(STEPS + 1):
                at = pl.ds(pl.multiple_of(g * BLOCK + start, 8), 8)
                a, c, d = cross[at, :], spread[at, :], weigh[at, :]
                for k in range(K):
                    there = pl.ds(g * WINDOW + start + lag[k], 8)
                    b, v = shifted[there, :], usable[there, :]
                    acc[k] = [acc[k][0] + a * b, acc[k][1] + c * v, acc[k][2] + d * (b * b)]
            for k in range(K):
                for n in range(3):
                    column = (n * TILES + part) * LANES
                    total[totals_at(k, t), column : column + LANES] = acc[k][n]
        return carry

    lax.fori_loop(0, GROUPS, tile, 0)
    first, second = halves_of(total[:, : 3 * LANES])
    gather = gather_matrix(0)
    out = dot(first, gather) + dot(second, gather)
    for n in range(1, 3):
        out += dot(total[:, 3 * n * LANES : 3 * (n + 1) * LANES].astype(jnp.bfloat16), gather_matrix(n))
    out_ref[...] = out.astype(jnp.bfloat16)


SCRATCH = ((3 * OWN_STRIDE, LANES), (2 * WINDOW_STRIDE, LANES), (K * GROUPS * 8, 9 * LANES))


def window_call(kernel, inputs, scratch, name, flops):
    vmem = pl.BlockSpec(memory_space=pltpu.VMEM)
    return pl.pallas_call(
        kernel,
        in_specs=[pl.BlockSpec(memory_space=pltpu.SMEM)] + [vmem] * (len(inputs) - 1),
        out_specs=vmem,
        out_shape=jax.ShapeDtypeStruct((K * GROUPS * 8, LANES), jnp.bfloat16),
        scratch_shapes=[pltpu.VMEM((rows, lanes), jnp.float32) for rows, lanes in scratch],
        name=name,
        **on_chip(28, flops),
    )(*inputs)


def finish_kernel(parts_ref, out_ref):
    lane = lax.broadcasted_iota(jnp.int32, (8, LANES), 1)
    halves = [[jnp.zeros((8, LANES), jnp.float32)] * 2 for _ in range(3)]
    for q in range(GROUPS):
        total = parts_ref[q * K].astype(jnp.float32)
        for device in range(1, K):
            total = total + parts_ref[q * K + device].astype(jnp.float32)
        fore = pltpu.roll(total, LANES - 3 * PER, 1)
        true = pltpu.roll(total, LANES - 6 * PER, 1)
        value = total / jnp.sqrt((fore + REG) * (true + REG))
        low, high = PER * q, PER * q + PER
        for part in range(3):
            moved = pltpu.roll(value, (PER * q - PER * part) % LANES, 1)
            for half in range(2):
                at = lane + half * LANES
                if low < (half + 1) * LANES and high > half * LANES:
                    halves[part][half] = jnp.where((at >= low) & (at < high), moved, halves[part][half])
    for part in range(3):
        out_ref[0, part * 8 : part * 8 + 8, :LANES] = halves[part][0]
        out_ref[0, part * 8 : part * 8 + 8, LANES:] = halves[part][1][:, : CHANNELS - LANES]


def finish(parts):
    vmem = pl.BlockSpec(memory_space=pltpu.VMEM)
    return pl.pallas_call(
        finish_kernel,
        in_specs=[vmem],
        out_specs=vmem,
        out_shape=jax.ShapeDtypeStruct((1, COLS, CHANNELS), jnp.float32),
        name="finish",
        **on_chip(4, 1_000_000),
    )(parts)


def local(prediction, observed_state, mean_state, usable_point_flags, eastward_offsets):
    place = np.arange(STEPS + 1)[:, None] * SIDE + np.arange(LANES)[None, :] // PER
    inside = (np.arange(LANES)[None, :] < PER * SIDE) & (place < ROWS)
    row = (lax.axis_index("lat") * ROWS + place).astype(jnp.float32)
    weight = jnp.cos(jnp.pi * ((row + 0.5) / (ROWS * lax.axis_size("lat")) - 0.5))
    weight = jnp.where(inside, weight, 0.0)
    flags = usable_point_flags.T
    around = ("y", "core")
    true = pack(observed_state, mean_state, flags)
    true = lax.all_to_all(true, around, 0, 0, tiled=True)
    count = lax.axis_size("z")
    following = lax.ppermute(true[:HALO], "z", [((i + 1) % count, i) for i in range(count)])
    fore = pack(prediction, mean_state, flags)
    fore = lax.all_to_all(fore, around, 0, 0, tiled=True)
    sums = window_call(
        sums_kernel,
        (eastward_offsets, weight, fore, true, following),
        SCRATCH,
        "lag_sums",
        20_000_000,
    )
    parts = sums.reshape(K * GROUPS, 8, LANES)
    parts = lax.all_to_all(parts, around + ("lat",), 0, 0, tiled=True)
    return finish(parts)


def solution(mesh):
    split = Mesh(mesh.devices.reshape(4, 8, 2, 8), ("z", "y", "core", "lat"))
    lon = ("z", "y", "core")
    placed = (P("lat", lon, None), P("lat", lon, None), P("lat", lon, None), P("lat", lon), P())
    return jax.shard_map(local, mesh=split, in_specs=placed, out_specs=P("lat", lon, None), check_vma=False)
```

```python
import jax
import jax.numpy as jnp
import numpy as np
from jax import lax
from jax.experimental import pallas as pl
from jax.experimental.pallas import tpu as pltpu
from jax.sharding import Mesh
from jax.sharding import PartitionSpec as P

REG = 0.001
K = 8
ROWS = 48
COLS = 24
TILES = COLS // 8
CHANNELS = 222
GROUPS = 16
PER = 14
SIDE = 9
STEPS = 5
TAIL = ROWS - STEPS * SIDE
PACKED = STEPS * COLS + 8
BLOCK = GROUPS * COLS
HALO = 14
WINDOW = BLOCK + HALO * COLS
MISSING = 1024.0
LANES = 128


def pack_kernel(field_ref, mean_ref, flags_ref, out_ref, field, mean, flags, low, mid, high, packed, arrived, leaving):
    def rows_of(g):
        return pl.ds(g * SIDE, SIDE if g < STEPS else TAIL)

    def fetch(g):
        rows = rows_of(g)
        return (
            pltpu.make_async_copy(field_ref.at[rows], field.at[rows], arrived.at[0, g]),
            pltpu.make_async_copy(mean_ref.at[rows], mean.at[rows], arrived.at[1, g]),
        )

    def leave(g):
        rows = pl.ds(g * COLS, COLS if g < STEPS else 8)
        return pltpu.make_async_copy(packed.at[:, rows, :], out_ref.at[:, rows, :], leaving.at[g])

    fetch_flags = pltpu.make_async_copy(flags_ref, flags, arrived.at[2, 0])
    fetch_flags.start()
    for g in range(STEPS + 1):
        for copy in fetch(g):
            copy.start()
    lane = lax.broadcasted_iota(jnp.int32, (8, LANES), 1)
    pad = jnp.zeros((COLS, 2 * LANES - CHANNELS), jnp.float32)
    fetch_flags.wait()
    valid = flags[...].astype(jnp.float32)

    def anomaly(row, keep):
        left = field[row, :, :LANES].astype(jnp.float32) - mean[row, :, :LANES].astype(jnp.float32)
        right = field[row, :, LANES:].astype(jnp.float32) - mean[row, :, LANES:].astype(jnp.float32)
        keep = jnp.broadcast_to(keep, (COLS, LANES)) > 0.5
        return jnp.where(keep, left, MISSING), jnp.where(keep, jnp.concatenate([right, pad], axis=1), MISSING)

    def place(turn, at, part, left, right):
        left, right = pltpu.roll(left, PER * at, 1), pltpu.roll(right, PER * at, 1)
        low[turn, at, part], high[turn, at, part] = left, right
        mid[turn, at, part] = jnp.where(((lane - PER * at) & (LANES - 1)) >= 9 * PER, left, right)

    def take(g):
        for copy in fetch(g):
            copy.wait()
        count = SIDE if g < STEPS else TAIL
        for row in range(count):
            at = g * SIDE + row
            left, right = anomaly(at, valid[:, at : at + 1])
            for part in range(TILES):
                slot, tile = (row, part) if g < STEPS else (part * TAIL + row, 0)
                rows = slice(part * 8, part * 8 + 8)
                place(g % 2, slot, tile, left[rows], right[rows])

    def emit(g):
        for q in range(GROUPS):
            source = low if q < 9 else mid if q == 9 else high
            slot = (lane - PER * q) & (LANES - 1)
            for part in range(TILES if g < STEPS else 1):
                acc = source[g % 2, 0, part]
                for at in range(1, SIDE):
                    acc = jnp.where(slot >= PER * at, source[g % 2, at, part], acc)
                moved = pltpu.roll(acc, -PER * q % LANES, 1)
                packed[q, pl.ds(g * COLS + part * 8, 8), :] = moved.astype(jnp.bfloat16)
        leave(g).start()

    take(0)
    for g in range(STEPS + 1):
        if g < STEPS:
            take(g + 1)
        emit(g)
    for g in range(STEPS + 1):
        leave(g).wait()


def on_chip(mib, flops):
    return dict(
        compiler_params=pltpu.CompilerParams(vmem_limit_bytes=mib * 1024 * 1024),
        cost_estimate=pl.CostEstimate(flops=flops, bytes_accessed=2_000_000, transcendentals=0),
    )


def pack(field, mean, flags):
    anywhere = pl.BlockSpec(memory_space=pl.ANY)
    return pl.pallas_call(
        pack_kernel,
        in_specs=[anywhere] * 3,
        out_specs=anywhere,
        out_shape=jax.ShapeDtypeStruct((GROUPS, PACKED, LANES), jnp.bfloat16),
        scratch_shapes=[pltpu.VMEM((ROWS, COLS, CHANNELS), jnp.bfloat16)] * 2
        + [pltpu.VMEM((COLS, ROWS), jnp.int32)]
        + [pltpu.VMEM((2, SIDE, TILES, 8, LANES), jnp.float32)] * 3
        + [pltpu.VMEM((GROUPS, PACKED, LANES), jnp.bfloat16)]
        + [pltpu.SemaphoreType.DMA((3, STEPS + 1)), pltpu.SemaphoreType.DMA((STEPS + 1,))],
        name="pack",
        **on_chip(62, 4_000_000),
    )(field, mean, flags)


def totals_at(k, t):
    return pl.ds(pl.multiple_of(((t % 2 * 8 + t // 2) * K + k) * 8, 8), 8)


def halves_of(value):
    first = value.astype(jnp.bfloat16)
    return first, (value - first.astype(jnp.float32)).astype(jnp.bfloat16)


OWN = (STEPS + 1) * BLOCK
OWN_STRIDE = OWN + 8
WINDOW_STRIDE = (STEPS + 1) * WINDOW + 16


def gather_matrix(n):
    row = lax.broadcasted_iota(jnp.int32, (3 * LANES, LANES), 0)
    lane = lax.broadcasted_iota(jnp.int32, (3 * LANES, LANES), 1)
    source = row & (LANES - 1)
    channel = source
    for at in range(1, SIDE + 1):
        channel = jnp.where(source >= PER * at, source - PER * at, channel)
    target = channel + PER * (TILES * n + row // LANES)
    return jnp.where((source < PER * SIDE) & (lane == target), 1.0, 0.0).astype(jnp.bfloat16)


def dot(a, b):
    return jnp.dot(a, b, preferred_element_type=jnp.float32)


def sums_kernel(offsets_ref, weight_ref, fore_ref, true_ref, next_ref, out_ref, held, window, total):
    cross, spread, weigh = (held.at[pl.ds(n * OWN_STRIDE, OWN)] for n in range(3))
    shifted, usable = (window.at[pl.ds(n * WINDOW_STRIDE, (STEPS + 1) * WINDOW)] for n in range(2))
    lane = lax.broadcasted_iota(jnp.int32, (8, LANES), 1)

    def unpack(source, first):
        def tile(g, part, p, value, fore):
            at = pl.ds(pl.multiple_of(g * WINDOW + first + p * COLS + part * 8, 8), 8)
            keep = value < MISSING / 2
            shifted[at, :] = jnp.where(keep, value, 0.0)
            usable[at, :] = jnp.where(keep, 1.0, 0.0)
            if first == 0:
                at = pl.ds(pl.multiple_of(g * BLOCK + p * COLS + part * 8, 8), 8)
                masked = jnp.where(keep, weight_ref[g : g + 1, :], 0.0)
                scaled = fore * masked
                weigh[at, :] = masked
                cross[at, :] = scaled
                spread[at, :] = scaled * fore

        def run(turn, carry):
            half = HALO // 2 if first else GROUPS // 2
            core, line = turn // half, turn % half
            source_block, p = core * 8 + line, line * 2 + core
            for g in range(STEPS):
                rows = slice(g * COLS, (g + 1) * COLS)
                value = source[source_block, rows, :].astype(jnp.float32)
                fore = fore_ref[source_block, rows, :].astype(jnp.float32) if first == 0 else value
                for part in range(TILES):
                    tile(g, part, p, value[part * 8 : part * 8 + 8], fore[part * 8 : part * 8 + 8])
            rows = slice(STEPS * COLS, PACKED)
            value = source[source_block, rows, :].astype(jnp.float32)
            fore = fore_ref[source_block, rows, :].astype(jnp.float32) if first == 0 else value
            for part in range(TILES):
                turn = -PER * TAIL * part % LANES
                moved = pltpu.roll(value, turn, 1) if part else value
                moved = jnp.where(lane < PER * TAIL, moved, MISSING)
                tile(STEPS, part, p, moved, pltpu.roll(fore, turn, 1) if part else fore)
            return carry

        return run

    lax.fori_loop(0, GROUPS, unpack(true_ref, 0), 0, unroll=8)
    lax.fori_loop(0, HALO, unpack(next_ref, BLOCK), 0, unroll=14)
    lag = [offsets_ref[k] for k in range(K)]

    def tile(t, carry):
        for part in range(TILES):
            start = t * COLS + part * 8
            acc = [[jnp.zeros((8, LANES), jnp.float32)] * 3 for _ in range(K)]
            for g in range(STEPS + 1):
                at = pl.ds(pl.multiple_of(g * BLOCK + start, 8), 8)
                a, c, d = cross[at, :], spread[at, :], weigh[at, :]
                for k in range(K):
                    there = pl.ds(g * WINDOW + start + lag[k], 8)
                    b, v = shifted[there, :], usable[there, :]
                    acc[k] = [acc[k][0] + a * b, acc[k][1] + c * v, acc[k][2] + d * (b * b)]
            for k in range(K):
                for n in range(3):
                    column = (n * TILES + part) * LANES
                    total[totals_at(k, t), column : column + LANES] = acc[k][n]
        return carry

    lax.fori_loop(0, GROUPS, tile, 0)
    first, second = halves_of(total[:, : 3 * LANES])
    gather = gather_matrix(0)
    out = dot(first, gather) + dot(second, gather)
    for n in range(1, 3):
        out += dot(total[:, 3 * n * LANES : 3 * (n + 1) * LANES].astype(jnp.bfloat16), gather_matrix(n))
    out_ref[...] = out.astype(jnp.bfloat16)


SCRATCH = ((3 * OWN_STRIDE, LANES), (2 * WINDOW_STRIDE, LANES), (K * GROUPS * 8, 9 * LANES))


def window_call(kernel, inputs, scratch, name, flops):
    vmem = pl.BlockSpec(memory_space=pltpu.VMEM)
    return pl.pallas_call(
        kernel,
        in_specs=[pl.BlockSpec(memory_space=pltpu.SMEM)] + [vmem] * (len(inputs) - 1),
        out_specs=vmem,
        out_shape=jax.ShapeDtypeStruct((K * GROUPS * 8, LANES), jnp.bfloat16),
        scratch_shapes=[pltpu.VMEM((rows, lanes), jnp.float32) for rows, lanes in scratch],
        name=name,
        **on_chip(28, flops),
    )(*inputs)


def finish_kernel(parts_ref, out_ref):
    lane = lax.broadcasted_iota(jnp.int32, (8, LANES), 1)
    halves = [[jnp.zeros((8, LANES), jnp.float32)] * 2 for _ in range(3)]
    for q in range(GROUPS):
        total = parts_ref[q * K].astype(jnp.float32)
        for device in range(1, K):
            total = total + parts_ref[q * K + device].astype(jnp.float32)
        fore = pltpu.roll(total, LANES - 3 * PER, 1)
        true = pltpu.roll(total, LANES - 6 * PER, 1)
        value = total / jnp.sqrt((fore + REG) * (true + REG))
        low, high = PER * q, PER * q + PER
        for part in range(3):
            moved = pltpu.roll(value, (PER * q - PER * part) % LANES, 1)
            for half in range(2):
                at = lane + half * LANES
                if low < (half + 1) * LANES and high > half * LANES:
                    halves[part][half] = jnp.where((at >= low) & (at < high), moved, halves[part][half])
    for part in range(3):
        out_ref[0, part * 8 : part * 8 + 8, :LANES] = halves[part][0]
        out_ref[0, part * 8 : part * 8 + 8, LANES:] = halves[part][1][:, : CHANNELS - LANES]


def finish(parts):
    vmem = pl.BlockSpec(memory_space=pltpu.VMEM)
    return pl.pallas_call(
        finish_kernel,
        in_specs=[vmem],
        out_specs=vmem,
        out_shape=jax.ShapeDtypeStruct((1, COLS, CHANNELS), jnp.float32),
        name="finish",
        **on_chip(4, 1_000_000),
    )(parts)


def local(prediction, observed_state, mean_state, usable_point_flags, eastward_offsets):
    place = np.arange(STEPS + 1)[:, None] * SIDE + np.arange(LANES)[None, :] // PER
    inside = (np.arange(LANES)[None, :] < PER * SIDE) & (place < ROWS)
    row = (lax.axis_index("lat") * ROWS + place).astype(jnp.float32)
    weight = jnp.cos(jnp.pi * ((row + 0.5) / (ROWS * lax.axis_size("lat")) - 0.5))
    weight = jnp.where(inside, weight, 0.0)
    flags = usable_point_flags.T
    around = ("core", "y")
    true = pack(observed_state, mean_state, flags)
    true = lax.all_to_all(true, around, 0, 0, tiled=True)
    count = lax.axis_size("z")
    following = lax.ppermute(true, "z", [((i + 1) % count, i) for i in range(count)])
    fore = pack(prediction, mean_state, flags)
    fore = lax.all_to_all(fore, around, 0, 0, tiled=True)
    sums = window_call(
        sums_kernel,
        (eastward_offsets, weight, fore, true, following),
        SCRATCH,
        "lag_sums",
        20_000_000,
    )
    parts = sums.reshape(K * GROUPS, 8, LANES)
    parts = lax.all_to_all(parts, around + ("lat",), 0, 0, tiled=True)
    return finish(parts)


def solution(mesh):
    split = Mesh(mesh.devices.reshape(4, 8, 2, 8), ("z", "y", "core", "lat"))
    lon = ("z", "y", "core")
    placed = (P("lat", lon, None), P("lat", lon, None), P("lat", lon, None), P("lat", lon), P())
    return jax.shard_map(local, mesh=split, in_specs=placed, out_specs=P("lat", lon, None), check_vma=False)
```

```python
import jax
import jax.numpy as jnp
import numpy as np
from jax import lax
from jax.experimental import pallas as pl
from jax.experimental.pallas import tpu as pltpu
from jax.sharding import Mesh
from jax.sharding import PartitionSpec as P

REG = 0.001
K = 8
ROWS = 48
COLS = 24
TILES = COLS // 8
CHANNELS = 222
GROUPS = 16
PER = 14
SIDE = 9
STEPS = 5
TAIL = ROWS - STEPS * SIDE
PACKED = STEPS * COLS + 8
BLOCK = GROUPS * COLS
HALO = 14
WINDOW = BLOCK + HALO * COLS
AROUND = [8, 9, 10, 11, 12, 13, 0, 1, 2, 3, 4, 5, 6, 7, 14, 15]
FIRST = (0 * 2 + 1) * K + 7
MISSING = 1024.0
LANES = 128


def pack_kernel(field_ref, mean_ref, flags_ref, out_ref, field, mean, flags, low, mid, high, packed, arrived, leaving):
    def rows_of(g):
        return pl.ds(g * SIDE, SIDE if g < STEPS else TAIL)

    def fetch(g):
        rows = rows_of(g)
        return (
            pltpu.make_async_copy(field_ref.at[rows], field.at[rows], arrived.at[0, g]),
            pltpu.make_async_copy(mean_ref.at[rows], mean.at[rows], arrived.at[1, g]),
        )

    def leave(g):
        rows = pl.ds(g * COLS, COLS if g < STEPS else 8)
        return pltpu.make_async_copy(packed.at[:, rows, :], out_ref.at[:, rows, :], leaving.at[g])

    fetch_flags = pltpu.make_async_copy(flags_ref, flags, arrived.at[2, 0])
    fetch_flags.start()
    for g in range(STEPS + 1):
        for copy in fetch(g):
            copy.start()
    lane = lax.broadcasted_iota(jnp.int32, (8, LANES), 1)
    pad = jnp.zeros((COLS, 2 * LANES - CHANNELS), jnp.float32)
    fetch_flags.wait()
    valid = flags[...].astype(jnp.float32)

    def anomaly(row, keep):
        left = field[row, :, :LANES].astype(jnp.float32) - mean[row, :, :LANES].astype(jnp.float32)
        right = field[row, :, LANES:].astype(jnp.float32) - mean[row, :, LANES:].astype(jnp.float32)
        keep = jnp.broadcast_to(keep, (COLS, LANES)) > 0.5
        return jnp.where(keep, left, MISSING), jnp.where(keep, jnp.concatenate([right, pad], axis=1), MISSING)

    def place(turn, at, part, left, right):
        left, right = pltpu.roll(left, PER * at, 1), pltpu.roll(right, PER * at, 1)
        low[turn, at, part], high[turn, at, part] = left, right
        mid[turn, at, part] = jnp.where(((lane - PER * at) & (LANES - 1)) >= 9 * PER, left, right)

    def take(g):
        for copy in fetch(g):
            copy.wait()
        count = SIDE if g < STEPS else TAIL
        for row in range(count):
            at = g * SIDE + row
            left, right = anomaly(at, valid[:, at : at + 1])
            for part in range(TILES):
                slot, tile = (row, part) if g < STEPS else (part * TAIL + row, 0)
                rows = slice(part * 8, part * 8 + 8)
                place(g % 2, slot, tile, left[rows], right[rows])

    def emit(g):
        for q in range(GROUPS):
            source = low if q < 9 else mid if q == 9 else high
            slot = (lane - PER * q) & (LANES - 1)
            for part in range(TILES if g < STEPS else 1):
                acc = source[g % 2, 0, part]
                for at in range(1, SIDE):
                    acc = jnp.where(slot >= PER * at, source[g % 2, at, part], acc)
                moved = pltpu.roll(acc, -PER * q % LANES, 1)
                packed[q, pl.ds(g * COLS + part * 8, 8), :] = moved.astype(jnp.bfloat16)
        leave(g).start()

    take(0)
    for g in range(STEPS + 1):
        if g < STEPS:
            take(g + 1)
        emit(g)
    for g in range(STEPS + 1):
        leave(g).wait()


def on_chip(mib, flops):
    return dict(
        compiler_params=pltpu.CompilerParams(vmem_limit_bytes=mib * 1024 * 1024),
        cost_estimate=pl.CostEstimate(flops=flops, bytes_accessed=2_000_000, transcendentals=0),
    )


def pack(field, mean, flags):
    anywhere = pl.BlockSpec(memory_space=pl.ANY)
    return pl.pallas_call(
        pack_kernel,
        in_specs=[anywhere] * 3,
        out_specs=anywhere,
        out_shape=jax.ShapeDtypeStruct((GROUPS, PACKED, LANES), jnp.bfloat16),
        scratch_shapes=[pltpu.VMEM((ROWS, COLS, CHANNELS), jnp.bfloat16)] * 2
        + [pltpu.VMEM((COLS, ROWS), jnp.int32)]
        + [pltpu.VMEM((2, SIDE, TILES, 8, LANES), jnp.float32)] * 3
        + [pltpu.VMEM((GROUPS, PACKED, LANES), jnp.bfloat16)]
        + [pltpu.SemaphoreType.DMA((3, STEPS + 1)), pltpu.SemaphoreType.DMA((STEPS + 1,))],
        name="pack",
        **on_chip(62, 4_000_000),
    )(field, mean, flags)


def totals_at(k, t):
    return pl.ds(pl.multiple_of(((t * K + k - FIRST) & (GROUPS * K - 1)) * 8, 8), 8)


def halves_of(value):
    first = value.astype(jnp.bfloat16)
    return first, (value - first.astype(jnp.float32)).astype(jnp.bfloat16)


OWN = (STEPS + 1) * BLOCK
OWN_STRIDE = OWN + 8
WINDOW_STRIDE = (STEPS + 1) * WINDOW + 16


def gather_matrix(n):
    row = lax.broadcasted_iota(jnp.int32, (3 * LANES, LANES), 0)
    lane = lax.broadcasted_iota(jnp.int32, (3 * LANES, LANES), 1)
    source = row & (LANES - 1)
    channel = source
    for at in range(1, SIDE + 1):
        channel = jnp.where(source >= PER * at, source - PER * at, channel)
    target = channel + PER * (TILES * n + row // LANES)
    return jnp.where((source < PER * SIDE) & (lane == target), 1.0, 0.0).astype(jnp.bfloat16)


def dot(a, b):
    return jnp.dot(a, b, preferred_element_type=jnp.float32)


def sums_kernel(offsets_ref, weight_ref, fore_ref, true_ref, next_ref, out_ref, held, window, total):
    cross, spread, weigh = (held.at[pl.ds(n * OWN_STRIDE, OWN)] for n in range(3))
    shifted, usable = (window.at[pl.ds(n * WINDOW_STRIDE, (STEPS + 1) * WINDOW)] for n in range(2))
    lane = lax.broadcasted_iota(jnp.int32, (8, LANES), 1)

    def unpack(source, first):
        def tile(g, part, p, value, fore):
            at = pl.ds(g * WINDOW + first + p * COLS + part * 8, 8)
            keep = value < MISSING / 2
            shifted[at, :] = jnp.where(keep, value, 0.0)
            usable[at, :] = jnp.where(keep, 1.0, 0.0)
            if first == 0:
                at = pl.ds(g * BLOCK + p * COLS + part * 8, 8)
                masked = jnp.where(keep, weight_ref[g : g + 1, :], 0.0)
                scaled = fore * masked
                weigh[at, :] = masked
                cross[at, :] = scaled
                spread[at, :] = scaled * fore

        for turn in range(source.shape[0]):
            p = AROUND[turn]
            for g in range(STEPS):
                rows = slice(g * COLS, (g + 1) * COLS)
                value = source[turn, rows, :].astype(jnp.float32)
                fore = fore_ref[turn, rows, :].astype(jnp.float32) if first == 0 else value
                for part in range(TILES):
                    tile(g, part, p, value[part * 8 : part * 8 + 8], fore[part * 8 : part * 8 + 8])
            rows = slice(STEPS * COLS, PACKED)
            value = source[turn, rows, :].astype(jnp.float32)
            fore = fore_ref[turn, rows, :].astype(jnp.float32) if first == 0 else value
            for part in range(TILES):
                shift = -PER * TAIL * part % LANES
                moved = pltpu.roll(value, shift, 1) if part else value
                moved = jnp.where(lane < PER * TAIL, moved, MISSING)
                tile(STEPS, part, p, moved, pltpu.roll(fore, shift, 1) if part else fore)

    unpack(true_ref, 0)
    unpack(next_ref, BLOCK)
    lag = [offsets_ref[k] for k in range(K)]

    def tile(t, carry):
        for part in range(TILES):
            start = t * COLS + part * 8
            acc = [[jnp.zeros((8, LANES), jnp.float32)] * 3 for _ in range(K)]
            for g in range(STEPS + 1):
                at = pl.ds(pl.multiple_of(g * BLOCK + start, 8), 8)
                a, c, d = cross[at, :], spread[at, :], weigh[at, :]
                for k in range(K):
                    there = pl.ds(g * WINDOW + start + lag[k], 8)
                    b, v = shifted[there, :], usable[there, :]
                    acc[k] = [acc[k][0] + a * b, acc[k][1] + c * v, acc[k][2] + d * (b * b)]
            for k in range(K):
                for n in range(3):
                    column = (n * TILES + part) * LANES
                    total[totals_at(k, t), column : column + LANES] = acc[k][n]
        return carry

    lax.fori_loop(0, GROUPS, tile, 0)
    first, second = halves_of(total[:, : 3 * LANES])
    gather = gather_matrix(0)
    out = dot(first, gather) + dot(second, gather)
    for n in range(1, 3):
        out += dot(total[:, 3 * n * LANES : 3 * (n + 1) * LANES].astype(jnp.bfloat16), gather_matrix(n))
    out_ref[...] = out.astype(jnp.bfloat16)


SCRATCH = ((3 * OWN_STRIDE, LANES), (2 * WINDOW_STRIDE, LANES), (K * GROUPS * 8, 9 * LANES))


def window_call(kernel, inputs, scratch, name, flops):
    vmem = pl.BlockSpec(memory_space=pltpu.VMEM)
    return pl.pallas_call(
        kernel,
        in_specs=[pl.BlockSpec(memory_space=pltpu.SMEM)] + [vmem] * (len(inputs) - 1),
        out_specs=vmem,
        out_shape=jax.ShapeDtypeStruct((K * GROUPS * 8, LANES), jnp.bfloat16),
        scratch_shapes=[pltpu.VMEM((rows, lanes), jnp.float32) for rows, lanes in scratch],
        name=name,
        **on_chip(28, flops),
    )(*inputs)


def finish_kernel(parts_ref, out_ref):
    lane = lax.broadcasted_iota(jnp.int32, (8, LANES), 1)
    halves = [[jnp.zeros((8, LANES), jnp.float32)] * 2 for _ in range(3)]
    for q in range(GROUPS):
        came = [(AROUND[q] * K + device - FIRST) % (GROUPS * K) for device in range(K)]
        total = parts_ref[came[0]].astype(jnp.float32)
        for at in came[1:]:
            total = total + parts_ref[at].astype(jnp.float32)
        fore = pltpu.roll(total, LANES - 3 * PER, 1)
        true = pltpu.roll(total, LANES - 6 * PER, 1)
        value = total / jnp.sqrt((fore + REG) * (true + REG))
        low, high = PER * q, PER * q + PER
        for part in range(3):
            moved = pltpu.roll(value, (PER * q - PER * part) % LANES, 1)
            for half in range(2):
                at = lane + half * LANES
                if low < (half + 1) * LANES and high > half * LANES:
                    halves[part][half] = jnp.where((at >= low) & (at < high), moved, halves[part][half])
    for part in range(3):
        out_ref[0, part * 8 : part * 8 + 8, :LANES] = halves[part][0]
        out_ref[0, part * 8 : part * 8 + 8, LANES:] = halves[part][1][:, : CHANNELS - LANES]


def finish(parts):
    vmem = pl.BlockSpec(memory_space=pltpu.VMEM)
    return pl.pallas_call(
        finish_kernel,
        in_specs=[vmem],
        out_specs=vmem,
        out_shape=jax.ShapeDtypeStruct((1, COLS, CHANNELS), jnp.float32),
        name="finish",
        **on_chip(4, 1_000_000),
    )(parts)


def local(prediction, observed_state, mean_state, usable_point_flags, eastward_offsets):
    place = np.arange(STEPS + 1)[:, None] * SIDE + np.arange(LANES)[None, :] // PER
    inside = (np.arange(LANES)[None, :] < PER * SIDE) & (place < ROWS)
    row = (lax.axis_index("lat") * ROWS + place).astype(jnp.float32)
    weight = jnp.cos(jnp.pi * ((row + 0.5) / (ROWS * lax.axis_size("lat")) - 0.5))
    weight = jnp.where(inside, weight, 0.0)
    flags = usable_point_flags.T
    around = ("y", "core")
    true = pack(observed_state, mean_state, flags)
    true = lax.all_to_all(true, around, 0, 0, tiled=True, axis_index_groups=[AROUND])
    count = lax.axis_size("z")
    following = lax.ppermute(true[:HALO], "z", [((i + 1) % count, i) for i in range(count)])
    fore = pack(prediction, mean_state, flags)
    fore = lax.all_to_all(fore, around, 0, 0, tiled=True, axis_index_groups=[AROUND])
    sums = window_call(
        sums_kernel,
        (eastward_offsets, weight, fore, true, following),
        SCRATCH,
        "lag_sums",
        20_000_000,
    )
    parts = sums.reshape(K * GROUPS, 8, LANES)
    turned = [(i + FIRST) % (GROUPS * K) for i in range(GROUPS * K)]
    parts = lax.all_to_all(parts, around + ("lat",), 0, 0, tiled=True, axis_index_groups=[turned])
    return finish(parts)


def solution(mesh):
    split = Mesh(mesh.devices.reshape(4, 8, 2, 8), ("z", "y", "core", "lat"))
    lon = ("z", "y", "core")
    placed = (P("lat", lon, None), P("lat", lon, None), P("lat", lon, None), P("lat", lon), P())
    return jax.shard_map(local, mesh=split, in_specs=placed, out_specs=P("lat", lon, None), check_vma=False)
```

```python
import jax
import jax.numpy as jnp
import numpy as np
from jax import lax
from jax.experimental import pallas as pl
from jax.experimental.pallas import tpu as pltpu
from jax.sharding import Mesh
from jax.sharding import PartitionSpec as P

REG = 0.001
K = 8
ROWS = 48
COLS = 24
TILES = COLS // 8
CHANNELS = 222
GROUPS = 16
PER = 14
SIDE = 9
STEPS = 5
TAIL = ROWS - STEPS * SIDE
PACKED = STEPS * COLS + 8
BLOCK = GROUPS * COLS
HALO = 14
WINDOW = BLOCK + HALO * COLS
AROUND = [9, 8, 10, 11, 12, 13, 0, 1, 2, 3, 4, 5, 6, 7, 14, 15]
FIRST = (4 * 2 + 1) * K + 5
MISSING = 1024.0
LANES = 128


def pack_kernel(field_ref, mean_ref, flags_ref, out_ref, field, mean, flags, low, mid, high, packed, arrived, leaving):
    def rows_of(g):
        return pl.ds(g * SIDE, SIDE if g < STEPS else TAIL)

    def fetch(g):
        rows = rows_of(g)
        return (
            pltpu.make_async_copy(field_ref.at[rows], field.at[rows], arrived.at[0, g]),
            pltpu.make_async_copy(mean_ref.at[rows], mean.at[rows], arrived.at[1, g]),
        )

    def leave(g):
        rows = pl.ds(g * COLS, COLS if g < STEPS else 8)
        return pltpu.make_async_copy(packed.at[:, rows, :], out_ref.at[:, rows, :], leaving.at[g])

    fetch_flags = pltpu.make_async_copy(flags_ref, flags, arrived.at[2, 0])
    fetch_flags.start()
    for g in range(STEPS + 1):
        for copy in fetch(g):
            copy.start()
    lane = lax.broadcasted_iota(jnp.int32, (8, LANES), 1)
    pad = jnp.zeros((COLS, 2 * LANES - CHANNELS), jnp.float32)
    fetch_flags.wait()
    valid = flags[...].astype(jnp.float32)

    def anomaly(row, keep):
        left = field[row, :, :LANES].astype(jnp.float32) - mean[row, :, :LANES].astype(jnp.float32)
        right = field[row, :, LANES:].astype(jnp.float32) - mean[row, :, LANES:].astype(jnp.float32)
        keep = jnp.broadcast_to(keep, (COLS, LANES)) > 0.5
        return jnp.where(keep, left, MISSING), jnp.where(keep, jnp.concatenate([right, pad], axis=1), MISSING)

    def place(turn, at, part, left, right):
        left, right = pltpu.roll(left, PER * at, 1), pltpu.roll(right, PER * at, 1)
        low[turn, at, part], high[turn, at, part] = left, right
        mid[turn, at, part] = jnp.where(((lane - PER * at) & (LANES - 1)) >= 9 * PER, left, right)

    def take(g):
        for copy in fetch(g):
            copy.wait()
        count = SIDE if g < STEPS else TAIL
        for row in range(count):
            at = g * SIDE + row
            left, right = anomaly(at, valid[:, at : at + 1])
            for part in range(TILES):
                slot, tile = (row, part) if g < STEPS else (part * TAIL + row, 0)
                rows = slice(part * 8, part * 8 + 8)
                place(g % 2, slot, tile, left[rows], right[rows])

    def emit(g):
        for q in range(GROUPS):
            source = low if q < 9 else mid if q == 9 else high
            slot = (lane - PER * q) & (LANES - 1)
            for part in range(TILES if g < STEPS else 1):
                acc = source[g % 2, 0, part]
                for at in range(1, SIDE):
                    acc = jnp.where(slot >= PER * at, source[g % 2, at, part], acc)
                moved = pltpu.roll(acc, -PER * q % LANES, 1)
                packed[q, pl.ds(g * COLS + part * 8, 8), :] = moved.astype(jnp.bfloat16)
        leave(g).start()

    take(0)
    for g in range(STEPS + 1):
        if g < STEPS:
            take(g + 1)
        emit(g)
    for g in range(STEPS + 1):
        leave(g).wait()


def on_chip(mib, flops):
    return dict(
        compiler_params=pltpu.CompilerParams(vmem_limit_bytes=mib * 1024 * 1024),
        cost_estimate=pl.CostEstimate(flops=flops, bytes_accessed=2_000_000, transcendentals=0),
    )


def pack(field, mean, flags):
    anywhere = pl.BlockSpec(memory_space=pl.ANY)
    return pl.pallas_call(
        pack_kernel,
        in_specs=[anywhere] * 3,
        out_specs=anywhere,
        out_shape=jax.ShapeDtypeStruct((GROUPS, PACKED, LANES), jnp.bfloat16),
        scratch_shapes=[pltpu.VMEM((ROWS, COLS, CHANNELS), jnp.bfloat16)] * 2
        + [pltpu.VMEM((COLS, ROWS), jnp.int32)]
        + [pltpu.VMEM((2, SIDE, TILES, 8, LANES), jnp.float32)] * 3
        + [pltpu.VMEM((GROUPS, PACKED, LANES), jnp.bfloat16)]
        + [pltpu.SemaphoreType.DMA((3, STEPS + 1)), pltpu.SemaphoreType.DMA((STEPS + 1,))],
        name="pack",
        **on_chip(62, 4_000_000),
    )(field, mean, flags)


def totals_at(k, t):
    return pl.ds(pl.multiple_of(((t * K + k - FIRST) & (GROUPS * K - 1)) * 8, 8), 8)


def halves_of(value):
    first = value.astype(jnp.bfloat16)
    return first, (value - first.astype(jnp.float32)).astype(jnp.bfloat16)


OWN = (STEPS + 1) * BLOCK
OWN_STRIDE = OWN + 8
WINDOW_STRIDE = (STEPS + 1) * WINDOW + 16


def gather_matrix(n):
    row = lax.broadcasted_iota(jnp.int32, (3 * LANES, LANES), 0)
    lane = lax.broadcasted_iota(jnp.int32, (3 * LANES, LANES), 1)
    source = row & (LANES - 1)
    channel = source
    for at in range(1, SIDE + 1):
        channel = jnp.where(source >= PER * at, source - PER * at, channel)
    target = channel + PER * (TILES * n + row // LANES)
    return jnp.where((source < PER * SIDE) & (lane == target), 1.0, 0.0).astype(jnp.bfloat16)


def dot(a, b):
    return jnp.dot(a, b, preferred_element_type=jnp.float32)


def sums_kernel(offsets_ref, weight_ref, fore_ref, true_ref, next_ref, out_ref, held, window, total):
    cross, spread, weigh = (held.at[pl.ds(n * OWN_STRIDE, OWN)] for n in range(3))
    shifted, usable = (window.at[pl.ds(n * WINDOW_STRIDE, (STEPS + 1) * WINDOW)] for n in range(2))
    lane = lax.broadcasted_iota(jnp.int32, (8, LANES), 1)

    def unpack(source, first):
        def tile(g, part, p, value, fore):
            at = pl.ds(g * WINDOW + first + p * COLS + part * 8, 8)
            keep = value < MISSING / 2
            shifted[at, :] = jnp.where(keep, value, 0.0)
            usable[at, :] = jnp.where(keep, 1.0, 0.0)
            if first == 0:
                at = pl.ds(g * BLOCK + p * COLS + part * 8, 8)
                masked = jnp.where(keep, weight_ref[g : g + 1, :], 0.0)
                scaled = fore * masked
                weigh[at, :] = masked
                cross[at, :] = scaled
                spread[at, :] = scaled * fore

        for turn in range(source.shape[0]):
            p = AROUND[turn]
            for g in range(STEPS):
                rows = slice(g * COLS, (g + 1) * COLS)
                value = source[turn, rows, :].astype(jnp.float32)
                fore = fore_ref[turn, rows, :].astype(jnp.float32) if first == 0 else value
                for part in range(TILES):
                    tile(g, part, p, value[part * 8 : part * 8 + 8], fore[part * 8 : part * 8 + 8])
            rows = slice(STEPS * COLS, PACKED)
            value = source[turn, rows, :].astype(jnp.float32)
            fore = fore_ref[turn, rows, :].astype(jnp.float32) if first == 0 else value
            for part in range(TILES):
                shift = -PER * TAIL * part % LANES
                moved = pltpu.roll(value, shift, 1) if part else value
                moved = jnp.where(lane < PER * TAIL, moved, MISSING)
                tile(STEPS, part, p, moved, pltpu.roll(fore, shift, 1) if part else fore)

    unpack(true_ref, 0)
    unpack(next_ref, BLOCK)
    lag = [offsets_ref[k] for k in range(K)]

    def tile(t, carry):
        for part in range(TILES):
            start = t * COLS + part * 8
            acc = [[jnp.zeros((8, LANES), jnp.float32)] * 3 for _ in range(K)]
            for g in range(STEPS + 1):
                at = pl.ds(pl.multiple_of(g * BLOCK + start, 8), 8)
                a, c, d = cross[at, :], spread[at, :], weigh[at, :]
                for k in range(K):
                    there = pl.ds(g * WINDOW + start + lag[k], 8)
                    b, v = shifted[there, :], usable[there, :]
                    acc[k] = [acc[k][0] + a * b, acc[k][1] + c * v, acc[k][2] + d * (b * b)]
            for k in range(K):
                for n in range(3):
                    column = (n * TILES + part) * LANES
                    total[totals_at(k, t), column : column + LANES] = acc[k][n]
        return carry

    lax.fori_loop(0, GROUPS, tile, 0)
    first, second = halves_of(total[:, : 3 * LANES])
    gather = gather_matrix(0)
    out = dot(first, gather) + dot(second, gather)
    for n in range(1, 3):
        out += dot(total[:, 3 * n * LANES : 3 * (n + 1) * LANES].astype(jnp.bfloat16), gather_matrix(n))
    out_ref[...] = out.astype(jnp.bfloat16)


SCRATCH = ((3 * OWN_STRIDE, LANES), (2 * WINDOW_STRIDE, LANES), (K * GROUPS * 8, 9 * LANES))


def window_call(kernel, inputs, scratch, name, flops):
    vmem = pl.BlockSpec(memory_space=pltpu.VMEM)
    return pl.pallas_call(
        kernel,
        in_specs=[pl.BlockSpec(memory_space=pltpu.SMEM)] + [vmem] * (len(inputs) - 1),
        out_specs=vmem,
        out_shape=jax.ShapeDtypeStruct((K * GROUPS * 8, LANES), jnp.bfloat16),
        scratch_shapes=[pltpu.VMEM((rows, lanes), jnp.float32) for rows, lanes in scratch],
        name=name,
        **on_chip(28, flops),
    )(*inputs)


def finish_kernel(parts_ref, out_ref):
    lane = lax.broadcasted_iota(jnp.int32, (8, LANES), 1)
    halves = [[jnp.zeros((8, LANES), jnp.float32)] * 2 for _ in range(3)]
    for q in range(GROUPS):
        came = [(AROUND[q] * K + device - FIRST) % (GROUPS * K) for device in range(K)]
        total = parts_ref[came[0]].astype(jnp.float32)
        for at in came[1:]:
            total = total + parts_ref[at].astype(jnp.float32)
        fore = pltpu.roll(total, LANES - 3 * PER, 1)
        true = pltpu.roll(total, LANES - 6 * PER, 1)
        value = total / jnp.sqrt((fore + REG) * (true + REG))
        low, high = PER * q, PER * q + PER
        for part in range(3):
            moved = pltpu.roll(value, (PER * q - PER * part) % LANES, 1)
            for half in range(2):
                at = lane + half * LANES
                if low < (half + 1) * LANES and high > half * LANES:
                    halves[part][half] = jnp.where((at >= low) & (at < high), moved, halves[part][half])
    for part in range(3):
        out_ref[0, part * 8 : part * 8 + 8, :LANES] = halves[part][0]
        out_ref[0, part * 8 : part * 8 + 8, LANES:] = halves[part][1][:, : CHANNELS - LANES]


def finish(parts):
    vmem = pl.BlockSpec(memory_space=pltpu.VMEM)
    return pl.pallas_call(
        finish_kernel,
        in_specs=[vmem],
        out_specs=vmem,
        out_shape=jax.ShapeDtypeStruct((1, COLS, CHANNELS), jnp.float32),
        name="finish",
        **on_chip(4, 1_000_000),
    )(parts)


def local(prediction, observed_state, mean_state, usable_point_flags, eastward_offsets):
    place = np.arange(STEPS + 1)[:, None] * SIDE + np.arange(LANES)[None, :] // PER
    inside = (np.arange(LANES)[None, :] < PER * SIDE) & (place < ROWS)
    row = (lax.axis_index("lat") * ROWS + place).astype(jnp.float32)
    weight = jnp.cos(jnp.pi * ((row + 0.5) / (ROWS * lax.axis_size("lat")) - 0.5))
    weight = jnp.where(inside, weight, 0.0)
    flags = usable_point_flags.T
    around = ("y", "core")
    true = pack(observed_state, mean_state, flags)
    true = lax.all_to_all(true, around, 0, 0, tiled=True, axis_index_groups=[AROUND])
    count = lax.axis_size("z")
    following = lax.ppermute(true[:HALO], "z", [((i + 1) % count, i) for i in range(count)])
    fore = pack(prediction, mean_state, flags)
    fore = lax.all_to_all(fore, around, 0, 0, tiled=True, axis_index_groups=[AROUND])
    sums = window_call(
        sums_kernel,
        (eastward_offsets, weight, fore, true, following),
        SCRATCH,
        "lag_sums",
        20_000_000,
    )
    parts = sums.reshape(K * GROUPS, 8, LANES)
    turned = [(i + FIRST) % (GROUPS * K) for i in range(GROUPS * K)]
    parts = lax.all_to_all(parts, around + ("lat",), 0, 0, tiled=True, axis_index_groups=[turned])
    return finish(parts)


def solution(mesh):
    split = Mesh(mesh.devices.reshape(4, 8, 2, 8), ("z", "y", "core", "lat"))
    lon = ("z", "y", "core")
    placed = (P("lat", lon, None), P("lat", lon, None), P("lat", lon, None), P("lat", lon), P())
    return jax.shard_map(local, mesh=split, in_specs=placed, out_specs=P("lat", lon, None), check_vma=False)
```

```python
import functools

import jax
import jax.numpy as jnp
import numpy as np
from jax import lax
from jax.experimental import pallas as pl
from jax.experimental.pallas import tpu as pltpu
from jax.sharding import Mesh
from jax.sharding import PartitionSpec as P

REG = 0.001
K = 8
ROWS = 48
COLS = 24
TILES = COLS // 8
CHANNELS = 222
GROUPS = 16
PER = 14
SIDE = 9
STEPS = 5
TAIL = ROWS - STEPS * SIDE
PACKED = STEPS * COLS + 8
BLOCK = GROUPS * COLS
HALO = 14
WINDOW = BLOCK + HALO * COLS
AROUND = [9, 8, 10, 11, 12, 13, 0, 1, 2, 3, 4, 5, 6, 7, 14, 15]
NATURAL = list(range(16))
FIRST = (4 * 2 + 1) * K + 5
MISSING = 1024.0
LANES = 128


def pack_kernel(order, field_ref, mean_ref, flags_ref, out_ref, field, mean, flags, low, mid, high, packed, arrived, leaving):
    def rows_of(g):
        return pl.ds(g * SIDE, SIDE if g < STEPS else TAIL)

    def fetch(g):
        rows = rows_of(g)
        return (
            pltpu.make_async_copy(field_ref.at[rows], field.at[rows], arrived.at[0, g]),
            pltpu.make_async_copy(mean_ref.at[rows], mean.at[rows], arrived.at[1, g]),
        )

    def leave(g):
        rows = pl.ds(g * COLS, COLS if g < STEPS else 8)
        return pltpu.make_async_copy(packed.at[:, rows, :], out_ref.at[:, rows, :], leaving.at[g])

    fetch_flags = pltpu.make_async_copy(flags_ref, flags, arrived.at[2, 0])
    fetch_flags.start()
    for g in range(STEPS + 1):
        for copy in fetch(g):
            copy.start()
    lane = lax.broadcasted_iota(jnp.int32, (8, LANES), 1)
    pad = jnp.zeros((COLS, 2 * LANES - CHANNELS), jnp.float32)
    fetch_flags.wait()
    valid = flags[...].astype(jnp.float32)

    def anomaly(row, keep):
        left = field[row, :, :LANES].astype(jnp.float32) - mean[row, :, :LANES].astype(jnp.float32)
        right = field[row, :, LANES:].astype(jnp.float32) - mean[row, :, LANES:].astype(jnp.float32)
        keep = jnp.broadcast_to(keep, (COLS, LANES)) > 0.5
        return jnp.where(keep, left, MISSING), jnp.where(keep, jnp.concatenate([right, pad], axis=1), MISSING)

    def place(turn, at, part, left, right):
        left, right = pltpu.roll(left, PER * at, 1), pltpu.roll(right, PER * at, 1)
        low[turn, at, part], high[turn, at, part] = left, right
        mid[turn, at, part] = jnp.where(((lane - PER * at) & (LANES - 1)) >= 9 * PER, left, right)

    def take(g):
        for copy in fetch(g):
            copy.wait()
        count = SIDE if g < STEPS else TAIL
        for row in range(count):
            at = g * SIDE + row
            left, right = anomaly(at, valid[:, at : at + 1])
            for part in range(TILES):
                slot, tile = (row, part) if g < STEPS else (part * TAIL + row, 0)
                rows = slice(part * 8, part * 8 + 8)
                place(g % 2, slot, tile, left[rows], right[rows])

    def emit(g):
        for to in range(GROUPS):
            q = AROUND.index(order[to])
            source = low if q < 9 else mid if q == 9 else high
            slot = (lane - PER * q) & (LANES - 1)
            for part in range(TILES if g < STEPS else 1):
                acc = source[g % 2, 0, part]
                for at in range(1, SIDE):
                    acc = jnp.where(slot >= PER * at, source[g % 2, at, part], acc)
                moved = pltpu.roll(acc, -PER * q % LANES, 1)
                packed[to, pl.ds(g * COLS + part * 8, 8), :] = moved.astype(jnp.bfloat16)
        leave(g).start()

    take(0)
    for g in range(STEPS + 1):
        if g < STEPS:
            take(g + 1)
        emit(g)
    for g in range(STEPS + 1):
        leave(g).wait()


def on_chip(mib, flops):
    return dict(
        compiler_params=pltpu.CompilerParams(vmem_limit_bytes=mib * 1024 * 1024),
        cost_estimate=pl.CostEstimate(flops=flops, bytes_accessed=2_000_000, transcendentals=0),
    )


def pack(field, mean, flags, order):
    anywhere = pl.BlockSpec(memory_space=pl.ANY)
    return pl.pallas_call(
        functools.partial(pack_kernel, order),
        in_specs=[anywhere] * 3,
        out_specs=anywhere,
        out_shape=jax.ShapeDtypeStruct((GROUPS, PACKED, LANES), jnp.bfloat16),
        scratch_shapes=[pltpu.VMEM((ROWS, COLS, CHANNELS), jnp.bfloat16)] * 2
        + [pltpu.VMEM((COLS, ROWS), jnp.int32)]
        + [pltpu.VMEM((2, SIDE, TILES, 8, LANES), jnp.float32)] * 3
        + [pltpu.VMEM((GROUPS, PACKED, LANES), jnp.bfloat16)]
        + [pltpu.SemaphoreType.DMA((3, STEPS + 1)), pltpu.SemaphoreType.DMA((STEPS + 1,))],
        name="pack",
        **on_chip(62, 4_000_000),
    )(field, mean, flags)


def totals_at(k, t):
    return pl.ds(pl.multiple_of(((t * K + k - FIRST) & (GROUPS * K - 1)) * 8, 8), 8)


def halves_of(value):
    first = value.astype(jnp.bfloat16)
    return first, (value - first.astype(jnp.float32)).astype(jnp.bfloat16)


OWN = (STEPS + 1) * BLOCK
OWN_STRIDE = OWN + 8
WINDOW_STRIDE = (STEPS + 1) * WINDOW + 16


def gather_matrix(n):
    row = lax.broadcasted_iota(jnp.int32, (3 * LANES, LANES), 0)
    lane = lax.broadcasted_iota(jnp.int32, (3 * LANES, LANES), 1)
    source = row & (LANES - 1)
    channel = source
    for at in range(1, SIDE + 1):
        channel = jnp.where(source >= PER * at, source - PER * at, channel)
    target = channel + PER * (TILES * n + row // LANES)
    return jnp.where((source < PER * SIDE) & (lane == target), 1.0, 0.0).astype(jnp.bfloat16)


def dot(a, b):
    return jnp.dot(a, b, preferred_element_type=jnp.float32)


def sums_kernel(offsets_ref, weight_ref, fore_ref, true_ref, next_ref, out_ref, held, window, total):
    cross, spread, weigh = (held.at[pl.ds(n * OWN_STRIDE, OWN)] for n in range(3))
    shifted, usable = (window.at[pl.ds(n * WINDOW_STRIDE, (STEPS + 1) * WINDOW)] for n in range(2))
    lane = lax.broadcasted_iota(jnp.int32, (8, LANES), 1)

    def unpack(source, first):
        def tile(g, part, p, value, fore):
            at = pl.ds(g * WINDOW + first + p * COLS + part * 8, 8)
            keep = value < MISSING / 2
            shifted[at, :] = jnp.where(keep, value, 0.0)
            usable[at, :] = jnp.where(keep, 1.0, 0.0)
            if first == 0:
                at = pl.ds(g * BLOCK + p * COLS + part * 8, 8)
                masked = jnp.where(keep, weight_ref[g : g + 1, :], 0.0)
                scaled = fore * masked
                weigh[at, :] = masked
                cross[at, :] = scaled
                spread[at, :] = scaled * fore

        for turn in range(source.shape[0]):
            p = AROUND[turn]
            for g in range(STEPS):
                rows = slice(g * COLS, (g + 1) * COLS)
                value = source[turn, rows, :].astype(jnp.float32)
                fore = fore_ref[p, rows, :].astype(jnp.float32) if first == 0 else value
                for part in range(TILES):
                    tile(g, part, p, value[part * 8 : part * 8 + 8], fore[part * 8 : part * 8 + 8])
            rows = slice(STEPS * COLS, PACKED)
            value = source[turn, rows, :].astype(jnp.float32)
            fore = fore_ref[p, rows, :].astype(jnp.float32) if first == 0 else value
            for part in range(TILES):
                shift = -PER * TAIL * part % LANES
                moved = pltpu.roll(value, shift, 1) if part else value
                moved = jnp.where(lane < PER * TAIL, moved, MISSING)
                tile(STEPS, part, p, moved, pltpu.roll(fore, shift, 1) if part else fore)

    unpack(true_ref, 0)
    unpack(next_ref, BLOCK)
    lag = [offsets_ref[k] for k in range(K)]

    def tile(t, carry):
        for part in range(TILES):
            start = t * COLS + part * 8
            acc = [[jnp.zeros((8, LANES), jnp.float32)] * 3 for _ in range(K)]
            for g in range(STEPS + 1):
                at = pl.ds(pl.multiple_of(g * BLOCK + start, 8), 8)
                a, c, d = cross[at, :], spread[at, :], weigh[at, :]
                for k in range(K):
                    there = pl.ds(g * WINDOW + start + lag[k], 8)
                    b, v = shifted[there, :], usable[there, :]
                    acc[k] = [acc[k][0] + a * b, acc[k][1] + c * v, acc[k][2] + d * (b * b)]
            for k in range(K):
                for n in range(3):
                    column = (n * TILES + part) * LANES
                    total[totals_at(k, t), column : column + LANES] = acc[k][n]
        return carry

    lax.fori_loop(0, GROUPS, tile, 0)
    first, second = halves_of(total[:, : 3 * LANES])
    gather = gather_matrix(0)
    out = dot(first, gather) + dot(second, gather)
    for n in range(1, 3):
        out += dot(total[:, 3 * n * LANES : 3 * (n + 1) * LANES].astype(jnp.bfloat16), gather_matrix(n))
    out_ref[...] = out.astype(jnp.bfloat16)


SCRATCH = ((3 * OWN_STRIDE, LANES), (2 * WINDOW_STRIDE, LANES), (K * GROUPS * 8, 9 * LANES))


def window_call(kernel, inputs, scratch, name, flops):
    vmem = pl.BlockSpec(memory_space=pltpu.VMEM)
    return pl.pallas_call(
        kernel,
        in_specs=[pl.BlockSpec(memory_space=pltpu.SMEM)] + [vmem] * (len(inputs) - 1),
        out_specs=vmem,
        out_shape=jax.ShapeDtypeStruct((K * GROUPS * 8, LANES), jnp.bfloat16),
        scratch_shapes=[pltpu.VMEM((rows, lanes), jnp.float32) for rows, lanes in scratch],
        name=name,
        **on_chip(28, flops),
    )(*inputs)


def finish_kernel(parts_ref, out_ref):
    lane = lax.broadcasted_iota(jnp.int32, (8, LANES), 1)
    halves = [[jnp.zeros((8, LANES), jnp.float32)] * 2 for _ in range(3)]
    for q in range(GROUPS):
        came = [(AROUND[q] * K + device - FIRST) % (GROUPS * K) for device in range(K)]
        total = parts_ref[came[0]].astype(jnp.float32)
        for at in came[1:]:
            total = total + parts_ref[at].astype(jnp.float32)
        fore = pltpu.roll(total, LANES - 3 * PER, 1)
        true = pltpu.roll(total, LANES - 6 * PER, 1)
        value = total / jnp.sqrt((fore + REG) * (true + REG))
        low, high = PER * q, PER * q + PER
        for part in range(3):
            moved = pltpu.roll(value, (PER * q - PER * part) % LANES, 1)
            for half in range(2):
                at = lane + half * LANES
                if low < (half + 1) * LANES and high > half * LANES:
                    halves[part][half] = jnp.where((at >= low) & (at < high), moved, halves[part][half])
    for part in range(3):
        out_ref[0, part * 8 : part * 8 + 8, :LANES] = halves[part][0]
        out_ref[0, part * 8 : part * 8 + 8, LANES:] = halves[part][1][:, : CHANNELS - LANES]


def finish(parts):
    vmem = pl.BlockSpec(memory_space=pltpu.VMEM)
    return pl.pallas_call(
        finish_kernel,
        in_specs=[vmem],
        out_specs=vmem,
        out_shape=jax.ShapeDtypeStruct((1, COLS, CHANNELS), jnp.float32),
        name="finish",
        **on_chip(4, 1_000_000),
    )(parts)


def local(prediction, observed_state, mean_state, usable_point_flags, eastward_offsets):
    place = np.arange(STEPS + 1)[:, None] * SIDE + np.arange(LANES)[None, :] // PER
    inside = (np.arange(LANES)[None, :] < PER * SIDE) & (place < ROWS)
    row = (lax.axis_index("lat") * ROWS + place).astype(jnp.float32)
    weight = jnp.cos(jnp.pi * ((row + 0.5) / (ROWS * lax.axis_size("lat")) - 0.5))
    weight = jnp.where(inside, weight, 0.0)
    flags = usable_point_flags.T
    around = ("y", "core")
    true = pack(observed_state, mean_state, flags, AROUND)
    true = lax.all_to_all(true, around, 0, 0, tiled=True, axis_index_groups=[AROUND])
    count = lax.axis_size("z")
    following = lax.ppermute(true[:HALO], "z", [((i + 1) % count, i) for i in range(count)])
    fore = pack(prediction, mean_state, flags, NATURAL)
    fore = lax.all_to_all(fore, around, 0, 0, tiled=True, axis_index_groups=[NATURAL])
    sums = window_call(
        sums_kernel,
        (eastward_offsets, weight, fore, true, following),
        SCRATCH,
        "lag_sums",
        20_000_000,
    )
    parts = sums.reshape(K * GROUPS, 8, LANES)
    turned = [(i + FIRST) % (GROUPS * K) for i in range(GROUPS * K)]
    parts = lax.all_to_all(parts, around + ("lat",), 0, 0, tiled=True, axis_index_groups=[turned])
    return finish(parts)


def solution(mesh):
    split = Mesh(mesh.devices.reshape(4, 8, 2, 8), ("z", "y", "core", "lat"))
    lon = ("z", "y", "core")
    placed = (P("lat", lon, None), P("lat", lon, None), P("lat", lon, None), P("lat", lon), P())
    return jax.shard_map(local, mesh=split, in_specs=placed, out_specs=P("lat", lon, None), check_vma=False)
```

```python
import jax
import jax.numpy as jnp
import numpy as np
from jax import lax
from jax.experimental import pallas as pl
from jax.experimental.pallas import tpu as pltpu
from jax.sharding import Mesh
from jax.sharding import PartitionSpec as P

REG = 0.001
K = 8
ROWS = 48
COLS = 24
TILES = COLS // 8
CHANNELS = 222
GROUPS = 16
PER = 14
SIDE = 9
STEPS = 5
TAIL = ROWS - STEPS * SIDE
PACKED = STEPS * COLS + 8
BLOCK = GROUPS * COLS
HALO = 14
WINDOW = BLOCK + HALO * COLS
AROUND = [9, 8, 10, 11, 12, 13, 0, 1, 2, 3, 4, 5, 6, 7, 14, 15]
FIRST = 5
MISSING = 1024.0
LANES = 128


def pack_kernel(field_ref, mean_ref, flags_ref, out_ref, field, mean, flags, low, mid, high, packed, arrived, leaving):
    def rows_of(g):
        return pl.ds(g * SIDE, SIDE if g < STEPS else TAIL)

    def fetch(g):
        rows = rows_of(g)
        return (
            pltpu.make_async_copy(field_ref.at[rows], field.at[rows], arrived.at[0, g]),
            pltpu.make_async_copy(mean_ref.at[rows], mean.at[rows], arrived.at[1, g]),
        )

    def leave(g):
        rows = pl.ds(g * COLS, COLS if g < STEPS else 8)
        return pltpu.make_async_copy(packed.at[:, rows, :], out_ref.at[:, rows, :], leaving.at[g])

    fetch_flags = pltpu.make_async_copy(flags_ref, flags, arrived.at[2, 0])
    fetch_flags.start()
    for g in range(STEPS + 1):
        for copy in fetch(g):
            copy.start()
    lane = lax.broadcasted_iota(jnp.int32, (8, LANES), 1)
    pad = jnp.zeros((COLS, 2 * LANES - CHANNELS), jnp.float32)
    fetch_flags.wait()
    valid = flags[...].astype(jnp.float32)

    def anomaly(row, keep):
        left = field[row, :, :LANES].astype(jnp.float32) - mean[row, :, :LANES].astype(jnp.float32)
        right = field[row, :, LANES:].astype(jnp.float32) - mean[row, :, LANES:].astype(jnp.float32)
        keep = jnp.broadcast_to(keep, (COLS, LANES)) > 0.5
        return jnp.where(keep, left, MISSING), jnp.where(keep, jnp.concatenate([right, pad], axis=1), MISSING)

    def place(turn, at, part, left, right):
        left, right = pltpu.roll(left, PER * at, 1), pltpu.roll(right, PER * at, 1)
        low[turn, at, part], high[turn, at, part] = left, right
        mid[turn, at, part] = jnp.where(((lane - PER * at) & (LANES - 1)) >= 9 * PER, left, right)

    def take(g):
        for copy in fetch(g):
            copy.wait()
        count = SIDE if g < STEPS else TAIL
        for row in range(count):
            at = g * SIDE + row
            left, right = anomaly(at, valid[:, at : at + 1])
            for part in range(TILES):
                slot, tile = (row, part) if g < STEPS else (part * TAIL + row, 0)
                rows = slice(part * 8, part * 8 + 8)
                place(g % 2, slot, tile, left[rows], right[rows])

    def emit(g):
        for q in range(GROUPS):
            source = low if q < 9 else mid if q == 9 else high
            slot = (lane - PER * q) & (LANES - 1)
            for part in range(TILES if g < STEPS else 1):
                acc = source[g % 2, 0, part]
                for at in range(1, SIDE):
                    acc = jnp.where(slot >= PER * at, source[g % 2, at, part], acc)
                moved = pltpu.roll(acc, -PER * q % LANES, 1)
                packed[q, pl.ds(g * COLS + part * 8, 8), :] = moved.astype(jnp.bfloat16)
        leave(g).start()

    take(0)
    for g in range(STEPS + 1):
        if g < STEPS:
            take(g + 1)
        emit(g)
    for g in range(STEPS + 1):
        leave(g).wait()


def on_chip(mib, flops):
    return dict(
        compiler_params=pltpu.CompilerParams(vmem_limit_bytes=mib * 1024 * 1024),
        cost_estimate=pl.CostEstimate(flops=flops, bytes_accessed=2_000_000, transcendentals=0),
    )


def pack(field, mean, flags):
    anywhere = pl.BlockSpec(memory_space=pl.ANY)
    return pl.pallas_call(
        pack_kernel,
        in_specs=[anywhere] * 3,
        out_specs=anywhere,
        out_shape=jax.ShapeDtypeStruct((GROUPS, PACKED, LANES), jnp.bfloat16),
        scratch_shapes=[pltpu.VMEM((ROWS, COLS, CHANNELS), jnp.bfloat16)] * 2
        + [pltpu.VMEM((COLS, ROWS), jnp.int32)]
        + [pltpu.VMEM((2, SIDE, TILES, 8, LANES), jnp.float32)] * 3
        + [pltpu.VMEM((GROUPS, PACKED, LANES), jnp.bfloat16)]
        + [pltpu.SemaphoreType.DMA((3, STEPS + 1)), pltpu.SemaphoreType.DMA((STEPS + 1,))],
        name="pack",
        **on_chip(62, 4_000_000),
    )(field, mean, flags)


def totals_at(k, t):
    return pl.ds(pl.multiple_of(((k - FIRST) % K * GROUPS + t) * 8, 8), 8)


def halves_of(value):
    first = value.astype(jnp.bfloat16)
    return first, (value - first.astype(jnp.float32)).astype(jnp.bfloat16)


OWN = (STEPS + 1) * BLOCK
OWN_STRIDE = OWN + 8
WINDOW_STRIDE = (STEPS + 1) * WINDOW + 16


def gather_matrix(n):
    row = lax.broadcasted_iota(jnp.int32, (3 * LANES, LANES), 0)
    lane = lax.broadcasted_iota(jnp.int32, (3 * LANES, LANES), 1)
    source = row & (LANES - 1)
    channel = source
    for at in range(1, SIDE + 1):
        channel = jnp.where(source >= PER * at, source - PER * at, channel)
    target = channel + PER * (TILES * n + row // LANES)
    return jnp.where((source < PER * SIDE) & (lane == target), 1.0, 0.0).astype(jnp.bfloat16)


def dot(a, b):
    return jnp.dot(a, b, preferred_element_type=jnp.float32)


def sums_kernel(offsets_ref, weight_ref, fore_ref, true_ref, next_ref, out_ref, held, window, total):
    cross, spread, weigh = (held.at[pl.ds(n * OWN_STRIDE, OWN)] for n in range(3))
    shifted, usable = (window.at[pl.ds(n * WINDOW_STRIDE, (STEPS + 1) * WINDOW)] for n in range(2))
    lane = lax.broadcasted_iota(jnp.int32, (8, LANES), 1)

    def unpack(source, first):
        def tile(g, part, p, value, fore):
            at = pl.ds(g * WINDOW + first + p * COLS + part * 8, 8)
            keep = value < MISSING / 2
            shifted[at, :] = jnp.where(keep, value, 0.0)
            usable[at, :] = jnp.where(keep, 1.0, 0.0)
            if first == 0:
                at = pl.ds(g * BLOCK + p * COLS + part * 8, 8)
                masked = jnp.where(keep, weight_ref[g : g + 1, :], 0.0)
                scaled = fore * masked
                weigh[at, :] = masked
                cross[at, :] = scaled
                spread[at, :] = scaled * fore

        for turn in range(source.shape[0]):
            p = AROUND[turn]
            for g in range(STEPS):
                rows = slice(g * COLS, (g + 1) * COLS)
                value = source[turn, rows, :].astype(jnp.float32)
                fore = fore_ref[turn, rows, :].astype(jnp.float32) if first == 0 else value
                for part in range(TILES):
                    tile(g, part, p, value[part * 8 : part * 8 + 8], fore[part * 8 : part * 8 + 8])
            rows = slice(STEPS * COLS, PACKED)
            value = source[turn, rows, :].astype(jnp.float32)
            fore = fore_ref[turn, rows, :].astype(jnp.float32) if first == 0 else value
            for part in range(TILES):
                shift = -PER * TAIL * part % LANES
                moved = pltpu.roll(value, shift, 1) if part else value
                moved = jnp.where(lane < PER * TAIL, moved, MISSING)
                tile(STEPS, part, p, moved, pltpu.roll(fore, shift, 1) if part else fore)

    unpack(true_ref, 0)
    unpack(next_ref, BLOCK)
    lag = [offsets_ref[k] for k in range(K)]

    def tile(t, carry):
        for part in range(TILES):
            start = t * COLS + part * 8
            acc = [[jnp.zeros((8, LANES), jnp.float32)] * 3 for _ in range(K)]
            for g in range(STEPS + 1):
                at = pl.ds(pl.multiple_of(g * BLOCK + start, 8), 8)
                a, c, d = cross[at, :], spread[at, :], weigh[at, :]
                for k in range(K):
                    there = pl.ds(g * WINDOW + start + lag[k], 8)
                    b, v = shifted[there, :], usable[there, :]
                    acc[k] = [acc[k][0] + a * b, acc[k][1] + c * v, acc[k][2] + d * (b * b)]
            for k in range(K):
                for n in range(3):
                    column = (n * TILES + part) * LANES
                    total[totals_at(k, t), column : column + LANES] = acc[k][n]
        return carry

    lax.fori_loop(0, GROUPS, tile, 0)
    first, second = halves_of(total[:, : 3 * LANES])
    gather = gather_matrix(0)
    out = dot(first, gather) + dot(second, gather)
    for n in range(1, 3):
        out += dot(total[:, 3 * n * LANES : 3 * (n + 1) * LANES].astype(jnp.bfloat16), gather_matrix(n))
    out_ref[...] = out.astype(jnp.bfloat16)


SCRATCH = ((3 * OWN_STRIDE, LANES), (2 * WINDOW_STRIDE, LANES), (K * GROUPS * 8, 9 * LANES))


def window_call(kernel, inputs, scratch, name, flops):
    vmem = pl.BlockSpec(memory_space=pltpu.VMEM)
    return pl.pallas_call(
        kernel,
        in_specs=[pl.BlockSpec(memory_space=pltpu.SMEM)] + [vmem] * (len(inputs) - 1),
        out_specs=vmem,
        out_shape=jax.ShapeDtypeStruct((K * GROUPS * 8, LANES), jnp.bfloat16),
        scratch_shapes=[pltpu.VMEM((rows, lanes), jnp.float32) for rows, lanes in scratch],
        name=name,
        **on_chip(28, flops),
    )(*inputs)


def correlate_kernel(parts_ref, out_ref):
    for block in range(GROUPS):
        total = parts_ref[0, block].astype(jnp.float32)
        for device in range(1, K):
            total = total + parts_ref[device, block].astype(jnp.float32)
        fore = pltpu.roll(total, LANES - 3 * PER, 1)
        true = pltpu.roll(total, LANES - 6 * PER, 1)
        out_ref[AROUND.index(block)] = total / jnp.sqrt((fore + REG) * (true + REG))


def finish_kernel(values_ref, out_ref):
    lane = lax.broadcasted_iota(jnp.int32, (8, LANES), 1)
    halves = [[jnp.zeros((8, LANES), jnp.float32)] * 2 for _ in range(3)]
    for q in range(GROUPS):
        value = values_ref[q]
        low, high = PER * q, PER * q + PER
        for part in range(3):
            moved = pltpu.roll(value, (PER * q - PER * part) % LANES, 1)
            for half in range(2):
                at = lane + half * LANES
                if low < (half + 1) * LANES and high > half * LANES:
                    halves[part][half] = jnp.where((at >= low) & (at < high), moved, halves[part][half])
    for part in range(3):
        out_ref[0, part * 8 : part * 8 + 8, :LANES] = halves[part][0]
        out_ref[0, part * 8 : part * 8 + 8, LANES:] = halves[part][1][:, : CHANNELS - LANES]


def small_call(kernel, value, shape, name):
    vmem = pl.BlockSpec(memory_space=pltpu.VMEM)
    return pl.pallas_call(
        kernel,
        in_specs=[vmem],
        out_specs=vmem,
        out_shape=jax.ShapeDtypeStruct(shape, jnp.float32),
        name=name,
        **on_chip(4, 1_000_000),
    )(value)


def local(prediction, observed_state, mean_state, usable_point_flags, eastward_offsets):
    place = np.arange(STEPS + 1)[:, None] * SIDE + np.arange(LANES)[None, :] // PER
    inside = (np.arange(LANES)[None, :] < PER * SIDE) & (place < ROWS)
    row = (lax.axis_index("lat") * ROWS + place).astype(jnp.float32)
    weight = jnp.cos(jnp.pi * ((row + 0.5) / (ROWS * lax.axis_size("lat")) - 0.5))
    weight = jnp.where(inside, weight, 0.0)
    flags = usable_point_flags.T
    around = ("y", "core")
    true = pack(observed_state, mean_state, flags)
    true = lax.all_to_all(true, around, 0, 0, tiled=True, axis_index_groups=[AROUND])
    count = lax.axis_size("z")
    following = lax.ppermute(true[:HALO], "z", [((i + 1) % count, i) for i in range(count)])
    fore = pack(prediction, mean_state, flags)
    fore = lax.all_to_all(fore, around, 0, 0, tiled=True, axis_index_groups=[AROUND])
    sums = window_call(
        sums_kernel,
        (eastward_offsets, weight, fore, true, following),
        SCRATCH,
        "lag_sums",
        20_000_000,
    )
    parts = sums.reshape(K, GROUPS, 8, LANES)
    turned = [(i + FIRST) % K for i in range(K)]
    parts = lax.all_to_all(parts, "lat", 0, 0, tiled=True, axis_index_groups=[turned])
    values = small_call(correlate_kernel, parts, (GROUPS, 8, LANES), "correlate")
    values = lax.all_to_all(values, around, 0, 0, tiled=True, axis_index_groups=[AROUND])
    return small_call(finish_kernel, values, (1, COLS, CHANNELS), "finish")


def solution(mesh):
    split = Mesh(mesh.devices.reshape(4, 8, 2, 8), ("z", "y", "core", "lat"))
    lon = ("z", "y", "core")
    placed = (P("lat", lon, None), P("lat", lon, None), P("lat", lon, None), P("lat", lon), P())
    return jax.shard_map(local, mesh=split, in_specs=placed, out_specs=P("lat", lon, None), check_vma=False)
```
